512 devices in a mesh: rep: 8 (over z_lo, x), shard: 64 (over z_hi, y, core).
Axes of the slice: x: 4, y: 8, z: 8 (z_hi: 4, z_lo: 2; z = z_hi * 2 + z_lo), core: 2. Of those that a mesh axis runs over, the one named last changes fastest.
Arguments:
- hidden: bfloat16 [196608, 256], P(('rep', 'shard')), may hold values from -24 to 24
- grad_out: bfloat16 [196608, 4096], P(('rep', 'shard')), may hold values from -6 to 6
- weight_band: bfloat16 [256, 4096], P('shard'), may hold values from -0.09375 to 0.09375
- error_feedback: float32 [8, 256, 4096], P('rep', 'shard'), may hold values from -2.1213202 to 2.1213202
- q_start: float32 [4096, 32], replicated, may hold values from -6 to 6
Outputs:
- update: float32 [256, 4096], P('shard')
- error_next: float32 [8, 256, 4096], P('rep', 'shard')
- q_next: float32 [4096, 32], replicated
- d_hidden: bfloat16 [196608, 256], P(('rep', 'shard'))
The draws below stay inside these ranges and needn't reach their ends.
All inputs are finite; a program needn't handle non-finite values.
Results may differ from the reference program's by a relative error of at most 0.0004.
Values may be sent and summed in bfloat16 or wider, within the bound.
No kernel may reach another device: no remote copies, remote signals or barrier semaphores. Data moves between devices by JAX's collectives and lax.ppermute only.
A program may use at most 64 MiB of HBM per device.

```python
import math
import jax
import jax.numpy as jnp
from jax import lax

D = 4096
TOK_DEV = 384
RANK = 32
POWER = 2
BUCKET = 256
TOKENS = 196608
N_REP = 8
N_SHARD = 64


def spiked(result, key, source, target, blocks, factor):
    owner, partner = [(jnp.arange(result.shape[dim]) // (result.shape[dim] // blocks)).reshape([-1 if axis == dim else 1 for axis in range(result.ndim)]) for dim in (source, target)]
    chosen = jax.random.permutation(key, blocks)[partner]
    strong = (owner == chosen) | (owner == (partner + blocks // 2) % blocks)
    return jnp.where(strong, factor * result, result)


def block_scale(key, shape, pieces, low, top_value):
    def one(axis_at, parts):
        steps = jax.random.uniform(jax.random.fold_in(jax.random.fold_in(key, 6), axis_at), (parts,), jnp.float32, low / len(pieces), top_value / len(pieces))
        return jnp.repeat(jnp.exp(steps), shape[axis_at] // parts).reshape((-1,) + (1,) * (len(shape) - axis_at - 1))

    gain = one(*pieces[0])
    for cut in pieces[1:]:
        gain = gain * one(*cut)
    return gain


def centred(key, dims, scale, reach, cuts=(), dtype=jnp.bfloat16):
    result = jax.random.normal(key, dims, jnp.float32) * scale
    if len(cuts) > 0:
        result = block_scale(key, dims, cuts, -0.22, 0.18) * result
    return jnp.clip(result, min=-reach, max=reach).astype(dtype)


def noise_with(key, shape, deviation, bound, cuts, heavy, dtype=jnp.bfloat16):
    array = deviation * jax.random.normal(key, shape, jnp.float32)
    if cuts:
        array = array * block_scale(key, shape, cuts, -0.22, 0.18)
    return jnp.clip(spiked(array, jax.random.fold_in(key, 3), *heavy), -bound, bound).astype(dtype)


def setup_inputs(seed: int = 0) -> dict:
    key_of = jax.random.split(jax.random.key(seed), 6)
    hidden = noise_with(key_of[0], (TOKENS, BUCKET), 1.0, 24.0, ((0, 512),), (0, 1, 256, 6.0))
    grad_out = centred(key_of[1], (TOKENS, D), 1.0, 6.0, ((0, 512),))
    weight_band = centred(key_of[2], (BUCKET, D), D ** -0.5, 0.09375, ((0, 64),))
    error_feedback = centred(key_of[3], (N_REP, BUCKET, D), (1.0 / N_REP ** 0.5), 2.1213202, ((0, 8), (1, 64)), jnp.float32)
    q_start = centred(key_of[4], (D, RANK), 1.0, 6.0, (), jnp.float32)
    return dict(hidden=hidden, grad_out=grad_out, weight_band=weight_band, error_feedback=error_feedback, q_start=q_start)


def orthonormal(matrix):
    gram_matrix = jnp.dot(matrix.T, matrix, precision=lax.Precision.HIGHEST)
    factor_low = jnp.linalg.cholesky(gram_matrix)
    return lax.linalg.triangular_solve(factor_low, matrix, left_side=False, lower=True, transpose_a=True)

def reference(hidden, grad_out, weight_band, error_feedback, q_start):
    group_tokens = TOK_DEV * N_SHARD
    grad_scale = 1.0 / math.sqrt(TOK_DEV * N_SHARD * N_REP)
    d_hidden = lax.dot_general(grad_out.astype(jnp.float32), weight_band.astype(jnp.float32), (((1,), (1,)), ((), ())), preferred_element_type=jnp.float32).astype(jnp.bfloat16)
    hidden_groups = hidden.reshape(N_REP, group_tokens, BUCKET)
    out_groups = grad_out.reshape(N_REP, group_tokens, D)

    def group_grad(operands):
        return lax.dot_general(operands[0].astype(jnp.float32), operands[1].astype(jnp.float32), (((0,), (0,)), ((), ())), preferred_element_type=jnp.float32) * grad_scale
    grads = lax.map(group_grad, (hidden_groups, out_groups))
    merged = grads + error_feedback
    summed = lax.optimization_barrier(jnp.sum(merged, axis=0))
    q_factor = q_start
    p_factor = None
    for round_index in range(POWER):
        q_hat = orthonormal(q_factor)
        p_factor = orthonormal(jnp.dot(summed, q_hat, precision=lax.Precision.HIGHEST))
        q_factor = jnp.dot(summed.T, p_factor, precision=lax.Precision.HIGHEST)
    update = jnp.dot(p_factor, q_factor.T, precision=lax.Precision.HIGHEST)
    error_next = merged - update / N_REP
    return (update, error_next, q_factor, d_hidden)
```

```python
import math

import jax
import jax.numpy as jnp
from jax import lax
from jax.experimental import pallas as pl
from jax.experimental.pallas import tpu as pltpu
from jax.sharding import Mesh
from jax.sharding import PartitionSpec as P

SHARD = ("shard_0", "shard_1", "shard_2")
REP_SHARD = ("rep", "shard_0", "shard_1", "shard_2")
CHIPS = ("shard_0", "shard_1")
CORE = "shard_2"
HIGHEST = lax.Precision.HIGHEST
VMEM = pl.BlockSpec(memory_space=pltpu.VMEM)
SMEM = pl.BlockSpec(memory_space=pltpu.SMEM)
F32 = jnp.float32


def nn(a, b):
    return lax.dot_general(
        a, b, (((1,), (0,)), ((), ())), precision=HIGHEST, preferred_element_type=F32
    )


def nt(a, b):
    return lax.dot_general(
        a, b, (((1,), (1,)), ((), ())), precision=HIGHEST, preferred_element_type=F32
    )


def inverse_factor(gram):
    n = gram.shape[0]
    rows = lax.broadcasted_iota(jnp.int32, (n, n), 0)
    cols = lax.broadcasted_iota(jnp.int32, (n, n), 1)
    a, b = gram, jnp.where(rows == cols, 1.0, 0.0).astype(F32)
    for j in range(n):
        down = jnp.where(rows[:, :1] > j, a[:, j : j + 1], 0.0)
        factor = down * (1.0 / a[j : j + 1, j : j + 1])
        a, b = a - factor * a[j : j + 1, :], b - factor * b[j : j + 1, :]
    pivots = jnp.sum(jnp.where(rows == cols, a, 0.0), axis=1, keepdims=True)
    return b * (1.0 / jnp.sqrt(pivots))


def orth_t(x):
    return nn(inverse_factor(nt(x, x)), x)


def call(kernel, out, *args, scalars=0):
    return pl.pallas_call(
        kernel,
        out_shape=out,
        in_specs=[SMEM] * scalars + [VMEM] * (len(args) - scalars),
        out_specs=jax.tree.map(lambda _: VMEM, out),
    )(*args)


def shaped(*shape, dtype=F32):
    return jax.ShapeDtypeStruct(shape, dtype)


def partial_kernel(scale, core, h_own, h_peer, g_own, g_peer, out):
    def term(h, g):
        return lax.dot_general(
            h[...], g[...], (((0,), (0,)), ((), ())), preferred_element_type=F32
        )

    out[...] = (term(h_own, g_own) + term(h_peer, g_peer)) * scale


def pair_partial(core, hidden, h_peer, grad_out, g_peer, scale):
    tokens, units = hidden.shape
    half = g_peer.shape[1]
    width = 512
    blocks = half // width

    def kernel(*refs):
        partial_kernel(scale, *refs)

    return pl.pallas_call(
        kernel,
        out_shape=shaped(units, half),
        grid_spec=pltpu.PrefetchScalarGridSpec(
            num_scalar_prefetch=1,
            grid=(blocks,),
            in_specs=[
                pl.BlockSpec((tokens, units), lambda i, c: (0, 0)),
                pl.BlockSpec((tokens, units), lambda i, c: (0, 0)),
                pl.BlockSpec((tokens, width), lambda i, c: (0, c[0] * blocks + i)),
                pl.BlockSpec((tokens, width), lambda i, c: (0, i)),
            ],
            out_specs=pl.BlockSpec((units, width), lambda i, c: (0, i)),
        ),
    )(core, hidden, h_peer, grad_out, g_peer)


def start_kernel(core, q_t, out):
    half = out.shape[1]
    inverse = inverse_factor(nt(q_t[...], q_t[...]))
    start = pl.multiple_of(core[0] * half, half)
    out[...] = nn(inverse, q_t[:, pl.ds(start, half)])


def left_kernel(q_t, summed, out):
    out[...] = nt(q_t[...], summed[...])


def first_kernel(y_own, y_peer, summed, p_out, y_out):
    p = orth_t(y_own[...] + y_peer[...])
    p_out[...] = p
    y_out[...] = nt(nn(p, summed[...]), summed[...])


def second_kernel(y_own, y_peer, p_old, summed, p_out, q_out):
    y = y_own[...] + y_peer[...]
    p = orth_t(nn(inverse_factor(nt(p_old[...], y)), y))
    p_out[...] = p
    q_out[...] = nn(p, summed[...])


def last_kernel(n_rep, core, row, q_own, q_peer, p_t, m_own, m_peer, q_out, update, error):
    rows, half = m_peer.shape
    width = p_t.shape[1]
    want = row[0] + lax.broadcasted_iota(jnp.int32, (8, width), 0)
    pick = jnp.where(lax.broadcasted_iota(jnp.int32, (8, width), 1) == want, 1.0, 0.0)
    p_rows = nt(pick.astype(F32), p_t[...])
    left = core[0] == 0
    for side in range(2):
        at = pl.ds(side * half, half)
        mine = left if side == 0 else jnp.logical_not(left)
        q = jnp.where(mine, q_own[...], q_peer[...])
        merged = jnp.where(mine, m_own[...], m_peer[...])
        q_out[:, at] = q
        step = nn(p_rows, q)[:rows]
        update[:, at] = step
        error[:, at] = merged - step * (1.0 / n_rep)


def swap(x):
    return lax.ppermute(x, CORE, [(0, 1), (1, 0)])


def side_of(x, side):
    half = x.shape[-1] // 2
    return lax.dynamic_slice_in_dim(x, side * half, half, x.ndim - 1)


def chip_rows(own, core):
    mine, other = side_of(own, core), swap(side_of(own, 1 - core))
    return jnp.where(
        core == 0, jnp.concatenate([mine, other], 0), jnp.concatenate([other, mine], 0)
    )


def to_all(x, axes):
    length = lax.axis_size(axes)
    return lax.all_to_all(jnp.broadcast_to(x[None], (length, *x.shape)), axes, 0, 0, tiled=True)


def body(hidden, grad_out, weight_band, error_feedback, q_start):
    n_rep = lax.axis_size("rep")
    chips = lax.axis_size(CHIPS)
    tokens, units = hidden.shape
    scale = 1.0 / math.sqrt(tokens * lax.axis_size(SHARD) * n_rep)
    core = lax.axis_index(CORE)
    core_s = core.astype(jnp.int32)[None]
    rows = weight_band.shape[0]
    half = grad_out.shape[1] // 2
    rank = q_start.shape[1]

    h_peer, g_peer = swap(hidden), swap(side_of(grad_out, 1 - core))
    feedback = chip_rows(error_feedback[0], core)
    weight = to_all(chip_rows(weight_band, core), CHIPS).reshape(units, half)
    q_t = call(start_kernel, shaped(rank, half), core_s, q_start.T, scalars=1)

    terms = pair_partial(core_s, hidden, h_peer, grad_out, g_peer, scale)
    terms = lax.all_to_all(terms.reshape(chips, -1, half), CHIPS, 0, 0, tiled=True)
    merged = terms.sum(axis=0) + feedback
    summed = to_all(merged, "rep").sum(axis=0)
    summed = to_all(summed, CHIPS).reshape(units, half)

    y = call(left_kernel, shaped(rank, units), q_t, summed)
    p_t, y = call(
        first_kernel, (shaped(rank, units), shaped(rank, units)), y, swap(y), summed
    )
    p_t, q_own = call(
        second_kernel, (shaped(rank, units), shaped(rank, half)), y, swap(y), p_t, summed
    )
    own_part = lax.dynamic_slice_in_dim(merged, core * rows, rows, 0)
    peer_part = swap(lax.dynamic_slice_in_dim(merged, (1 - core) * rows, rows, 0))
    row = (lax.axis_index(SHARD) * rows).astype(jnp.int32)[None]
    q_next, update, error = call(
        lambda *refs: last_kernel(n_rep, *refs),
        (shaped(rank, 2 * half), shaped(rows, 2 * half), shaped(rows, 2 * half)),
        core_s,
        row,
        q_own,
        swap(q_own),
        p_t,
        own_part,
        peer_part,
        scalars=2,
    )

    def back(g):
        return lax.dot_general(g, weight, (((1,), (1,)), ((), ())), preferred_element_type=F32)

    d_hidden = (back(side_of(grad_out, core)) + swap(back(g_peer))).astype(jnp.bfloat16)
    return (update, error[None], q_next.T, d_hidden)


def solution(mesh):
    finer = Mesh(
        mesh.devices.reshape(mesh.shape["rep"], 4, 8, 2), ("rep", "shard_0", "shard_1", "shard_2")
    )
    placed = (P(REP_SHARD, None), P(REP_SHARD, None), P(SHARD, None), P("rep", SHARD, None), P())
    return jax.shard_map(
        body,
        mesh=finer,
        in_specs=placed,
        out_specs=(P(SHARD, None), P("rep", SHARD, None), P(), P(REP_SHARD, None)),
        check_vma=False,
    )
```

```python
import math

import jax
import jax.numpy as jnp
from jax import lax
from jax.experimental import pallas as pl
from jax.experimental.pallas import tpu as pltpu
from jax.sharding import Mesh
from jax.sharding import PartitionSpec as P

SHARD = ("shard_0", "shard_1", "shard_2")
REP_SHARD = ("rep", "shard_0", "shard_1", "shard_2")
CHIPS = ("shard_0", "shard_1")
CORE = "shard_2"
HIGHEST = lax.Precision.HIGHEST
VMEM = pl.BlockSpec(memory_space=pltpu.VMEM)
SMEM = pl.BlockSpec(memory_space=pltpu.SMEM)
F32 = jnp.float32


def nn(a, b):
    return lax.dot_general(
        a, b, (((1,), (0,)), ((), ())), precision=HIGHEST, preferred_element_type=F32
    )


def nt(a, b):
    return lax.dot_general(
        a, b, (((1,), (1,)), ((), ())), precision=HIGHEST, preferred_element_type=F32
    )


def inverse_factor(gram):
    n = gram.shape[0]
    rows = lax.broadcasted_iota(jnp.int32, (n, n), 0)
    cols = lax.broadcasted_iota(jnp.int32, (n, n), 1)
    a, b = gram, jnp.where(rows == cols, 1.0, 0.0).astype(F32)
    for j in range(n):
        down = jnp.where(rows[:, :1] > j, a[:, j : j + 1], 0.0)
        factor = down * (1.0 / a[j : j + 1, j : j + 1])
        a, b = a - factor * a[j : j + 1, :], b - factor * b[j : j + 1, :]
    pivots = jnp.sum(jnp.where(rows == cols, a, 0.0), axis=1, keepdims=True)
    return b * (1.0 / jnp.sqrt(pivots))


def orth_t(x):
    return nn(inverse_factor(nt(x, x)), x)


def call(kernel, out, *args, scalars=0):
    return pl.pallas_call(
        kernel,
        out_shape=out,
        in_specs=[SMEM] * scalars + [VMEM] * (len(args) - scalars),
        out_specs=jax.tree.map(lambda _: VMEM, out),
    )(*args)


def shaped(*shape, dtype=F32):
    return jax.ShapeDtypeStruct(shape, dtype)


SPAN = 250.0
LN2 = math.log(2.0)
BLOCK = 512
TAIL = 128


def code(x):
    top = jnp.max(jnp.abs(x), axis=1, keepdims=True)
    top = jnp.maximum(top * 1.01, 1e-30).astype(jnp.bfloat16).astype(F32)
    level = jnp.sqrt(jnp.abs(x) * (1.0 / top))
    size = jnp.exp(level * (SPAN * LN2) - (SPAN * LN2 / 2))
    return jnp.where(x < 0, -size, size).astype(jnp.bfloat16), top


def decode(y, top):
    y = y.astype(F32)
    level = jnp.log(jnp.abs(y)) * (1.0 / (SPAN * LN2)) + 0.5
    size = level * level * top
    return jnp.where(y < 0, -size, size)


def pair_partial(core, hidden, h_peer, grad_out, g_peer, scale):
    tokens, units = hidden.shape
    half = g_peer.shape[1]
    blocks = half // BLOCK

    def kernel(core, h_own, h_peer, g_own, g_peer, out, tops):
        def term(h, g):
            return lax.dot_general(
                h[...], g[...], (((0,), (0,)), ((), ())), preferred_element_type=F32
            )

        i = pl.program_id(0)
        coded, top = code((term(h_own, g_own) + term(h_peer, g_peer)) * scale)
        out[:, pl.ds(pl.multiple_of(i * BLOCK, BLOCK), BLOCK)] = coded
        lane = lax.broadcasted_iota(jnp.int32, (units, TAIL), 1) // 32
        tops[...] = jnp.where(lane == i, top, tops[...])
        out[:, half:] = tops[...].astype(jnp.bfloat16)

    return pl.pallas_call(
        kernel,
        out_shape=shaped(units, half + TAIL, dtype=jnp.bfloat16),
        grid_spec=pltpu.PrefetchScalarGridSpec(
            num_scalar_prefetch=1,
            grid=(blocks,),
            in_specs=[
                pl.BlockSpec((tokens, units), lambda i, c: (0, 0)),
                pl.BlockSpec((tokens, units), lambda i, c: (0, 0)),
                pl.BlockSpec((tokens, BLOCK), lambda i, c: (0, c[0] * blocks + i)),
                pl.BlockSpec((tokens, BLOCK), lambda i, c: (0, i)),
            ],
            out_specs=pl.BlockSpec((units, half + TAIL), lambda i, c: (0, 0)),
            scratch_shapes=[pltpu.VMEM((units, TAIL), F32)],
        ),
    )(core, hidden, h_peer, grad_out, g_peer)


def merge_kernel(terms, feedback, merged, copies):
    half = feedback.shape[1]
    for j in range(half // BLOCK):
        at = pl.ds(j * BLOCK, BLOCK)
        total = feedback[:, at]
        for source in range(terms.shape[0]):
            tail = terms[source, :, half:].astype(F32)
            total = total + decode(terms[source, :, at], tail[:, 32 * j : 32 * j + 1])
        merged[:, at] = total
        for target in range(copies.shape[0]):
            copies[target, :, at] = total


def sum_kernel(merged, copies):
    half = merged.shape[2]
    tops = []
    for j in range(half // BLOCK):
        at = pl.ds(j * BLOCK, BLOCK)
        coded, top = code(jnp.sum(merged[:, :, at], axis=0))
        tops.append(jnp.broadcast_to(top, (top.shape[0], 32)))
        for target in range(copies.shape[0]):
            copies[target, :, at] = coded
    tail = jnp.concatenate(tops, axis=1).astype(jnp.bfloat16)
    for target in range(copies.shape[0]):
        copies[target, :, half:] = tail


def start_kernel(core, q_t, out):
    half = out.shape[1]
    inverse = inverse_factor(nt(q_t[...], q_t[...]))
    start = pl.multiple_of(core[0] * half, half)
    out[...] = nn(inverse, q_t[:, pl.ds(start, half)])


def left_kernel(q_t, coded, summed, y_out):
    rows, half = coded.shape[1], q_t.shape[1]
    for source in range(coded.shape[0]):
        tail = coded[source, :, half:].astype(F32)
        for j in range(half // BLOCK):
            at = pl.ds(j * BLOCK, BLOCK)
            summed[pl.ds(source * rows, rows), at] = decode(
                coded[source, :, at], tail[:, 32 * j : 32 * j + 1]
            )
    y_out[...] = nt(q_t[...], summed[...])


def first_kernel(y_own, y_peer, summed, p_out, y_out):
    p = orth_t(y_own[...] + y_peer[...])
    p_out[...] = p
    y_out[...] = nt(nn(p, summed[...]), summed[...])


def second_kernel(y_own, y_peer, p_old, summed, p_out, q_out):
    y = y_own[...] + y_peer[...]
    p = orth_t(nn(inverse_factor(nt(p_old[...], y)), y))
    p_out[...] = p
    q_out[...] = nn(p, summed[...])


def last_kernel(n_rep, core, row, q_own, q_peer, p_t, m_own, m_peer, q_out, update, error):
    rows, half = m_peer.shape
    width = p_t.shape[1]
    want = row[0] + lax.broadcasted_iota(jnp.int32, (8, width), 0)
    pick = jnp.where(lax.broadcasted_iota(jnp.int32, (8, width), 1) == want, 1.0, 0.0)
    p_rows = nt(pick.astype(F32), p_t[...])
    left = core[0] == 0
    for side in range(2):
        at = pl.ds(side * half, half)
        mine = left if side == 0 else jnp.logical_not(left)
        q = jnp.where(mine, q_own[...], q_peer[...])
        merged = jnp.where(mine, m_own[...], m_peer[...])
        q_out[:, at] = q
        step = nn(p_rows, q)[:rows]
        update[:, at] = step
        error[:, at] = merged - step * (1.0 / n_rep)


def swap(x):
    return lax.ppermute(x, CORE, [(0, 1), (1, 0)])


def side_of(x, side):
    half = x.shape[-1] // 2
    return lax.dynamic_slice_in_dim(x, side * half, half, x.ndim - 1)


def chip_rows(own, core):
    mine, other = side_of(own, core), swap(side_of(own, 1 - core))
    return jnp.where(
        core == 0, jnp.concatenate([mine, other], 0), jnp.concatenate([other, mine], 0)
    )


def exchange(blocks, axes):
    return lax.all_to_all(blocks, axes, 0, 0, tiled=True)


def to_all(x, axes):
    return exchange(jnp.broadcast_to(x[None], (lax.axis_size(axes), *x.shape)), axes)


def body(hidden, grad_out, weight_band, error_feedback, q_start):
    n_rep = lax.axis_size("rep")
    chips = lax.axis_size(CHIPS)
    tokens, units = hidden.shape
    scale = 1.0 / math.sqrt(tokens * lax.axis_size(SHARD) * n_rep)
    core = lax.axis_index(CORE)
    core_s = core.astype(jnp.int32)[None]
    rows = weight_band.shape[0]
    half = grad_out.shape[1] // 2
    rank = q_start.shape[1]

    h_peer, g_peer = swap(hidden), swap(side_of(grad_out, 1 - core))
    feedback = chip_rows(error_feedback[0], core)
    weight = chip_rows(weight_band, core)
    q_t = call(start_kernel, shaped(rank, half), core_s, q_start.T, scalars=1)

    terms = pair_partial(core_s, hidden, h_peer, grad_out, g_peer, scale)
    terms = exchange(terms.reshape(chips, -1, half + TAIL), CHIPS)
    merged, copies = call(
        merge_kernel,
        (shaped(2 * rows, half), shaped(n_rep, 2 * rows, half)),
        terms,
        feedback,
    )
    copies = call(
        sum_kernel,
        shaped(chips, 2 * rows, half + TAIL, dtype=jnp.bfloat16),
        exchange(copies, "rep"),
    )
    coded = exchange(copies, CHIPS)
    coded, weight = lax.optimization_barrier((coded, weight))
    weight = to_all(weight, CHIPS).reshape(units, half)
    summed, y = call(left_kernel, (shaped(units, half), shaped(rank, units)), q_t, coded)
    p_t, y = call(
        first_kernel, (shaped(rank, units), shaped(rank, units)), y, swap(y), summed
    )
    p_t, q_own = call(
        second_kernel, (shaped(rank, units), shaped(rank, half)), y, swap(y), p_t, summed
    )
    own_part = lax.dynamic_slice_in_dim(merged, core * rows, rows, 0)
    peer_part = swap(lax.dynamic_slice_in_dim(merged, (1 - core) * rows, rows, 0))
    row = (lax.axis_index(SHARD) * rows).astype(jnp.int32)[None]
    q_next, update, error = call(
        lambda *refs: last_kernel(n_rep, *refs),
        (shaped(rank, 2 * half), shaped(rows, 2 * half), shaped(rows, 2 * half)),
        core_s,
        row,
        q_own,
        swap(q_own),
        p_t,
        own_part,
        peer_part,
        scalars=2,
    )

    def back(g):
        return lax.dot_general(g, weight, (((1,), (1,)), ((), ())), preferred_element_type=F32)

    d_hidden = (back(side_of(grad_out, core)) + swap(back(g_peer))).astype(jnp.bfloat16)
    return (update, error[None], q_next.T, d_hidden)


def solution(mesh):
    finer = Mesh(
        mesh.devices.reshape(mesh.shape["rep"], 4, 8, 2), ("rep", "shard_0", "shard_1", "shard_2")
    )
    placed = (P(REP_SHARD, None), P(REP_SHARD, None), P(SHARD, None), P("rep", SHARD, None), P())
    return jax.shard_map(
        body,
        mesh=finer,
        in_specs=placed,
        out_specs=(P(SHARD, None), P("rep", SHARD, None), P(), P(REP_SHARD, None)),
        check_vma=False,
    )
```

```python
import math

import jax
import jax.numpy as jnp
from jax import lax
from jax.experimental import pallas as pl
from jax.experimental.pallas import tpu as pltpu
from jax.sharding import Mesh
from jax.sharding import PartitionSpec as P

SHARD = ("shard_0", "shard_1", "shard_2")
REP_SHARD = ("rep", "shard_0", "shard_1", "shard_2")
CHIPS = ("shard_0", "shard_1")
CORE = "shard_2"
HIGHEST = lax.Precision.HIGHEST
F32, BF16 = jnp.float32, jnp.bfloat16
SPAN = 250.0
LN2 = math.log(2.0)
BLOCK = 512
TAIL = 128
LANES = 32


def dot(a, b, over, precision=None):
    return lax.dot_general(
        a, b, ((over[:1], over[1:]), ((), ())), precision=precision, preferred_element_type=F32
    )


def nn(a, b):
    return dot(a, b, (1, 0), HIGHEST)


def nt(a, b):
    return dot(a, b, (1, 1), HIGHEST)


def parts(x):
    high = x.astype(BF16)
    return high, (x - high.astype(F32)).astype(BF16)


def dot3(a, b, over):
    return dot(a[0], b[0], over) + (dot(a[0], b[1], over) + dot(a[1], b[0], over))


def inverse_factor(gram):
    n = gram.shape[0]
    rows = lax.broadcasted_iota(jnp.int32, (n, n), 0)
    cols = lax.broadcasted_iota(jnp.int32, (n, n), 1)
    a, b = gram, jnp.where(rows == cols, 1.0, 0.0).astype(F32)
    for j in range(n):
        down = jnp.where(rows[:, :1] > j, a[:, j : j + 1], 0.0)
        factor = down * (1.0 / a[j : j + 1, j : j + 1])
        a, b = a - factor * a[j : j + 1, :], b - factor * b[j : j + 1, :]
    pivots = jnp.sum(jnp.where(rows == cols, a, 0.0), axis=1, keepdims=True)
    return b * (1.0 / jnp.sqrt(pivots))


def orth_t(x):
    return nn(inverse_factor(nt(x, x)), x)


def code(x):
    top = jnp.max(jnp.abs(x), axis=1, keepdims=True)
    top = jnp.maximum(top * 1.01, 1e-30).astype(BF16).astype(F32)
    level = jnp.sqrt(jnp.abs(x) * (1.0 / top))
    size = jnp.exp(level * (SPAN * LN2) - (SPAN * LN2 / 2))
    return jnp.where(x < 0, -size, size).astype(BF16), top


def decode(y, top):
    y = y.astype(F32)
    level = jnp.log(jnp.abs(y)) * (1.0 / (SPAN * LN2)) + 0.5
    size = level * level * top
    return jnp.where(y < 0, -size, size)


def tail_of(tops):
    wide = [jnp.broadcast_to(top, (top.shape[0], LANES)) for top in tops]
    return jnp.concatenate(wide, axis=1).astype(BF16)


def blocks_of(half):
    return [pl.ds(j * BLOCK, BLOCK) for j in range(half // BLOCK)]


def near(*shape, dtype=F32):
    return pltpu.VMEM(shape, dtype)


def far(*shape, dtype=F32):
    return jax.ShapeDtypeStruct(shape, dtype)


def call(kernel, out, *args, scalars=0, held=(), scratch=()):
    vmem = pl.BlockSpec(memory_space=pltpu.VMEM)
    smem = pl.BlockSpec(memory_space=pltpu.SMEM)
    hbm = pl.BlockSpec(memory_space=pltpu.HBM)
    kinds = [smem if i < scalars else hbm if i in held else vmem for i in range(len(args))]
    placed = [
        x if kind is smem else pltpu.with_memory_space_constraint(x, kind.memory_space)
        for x, kind in zip(args, kinds)
    ]
    return pl.pallas_call(
        kernel,
        out_shape=out,
        in_specs=kinds,
        out_specs=(vmem,) * len(out) if isinstance(out, tuple) else vmem,
        scratch_shapes=list(scratch),
        compiler_params=pltpu.CompilerParams(vmem_limit_bytes=24 << 20),
    )(*placed)


def partial_kernel(scale, h_own, h_peer, g_own, g_peer, out):
    half = g_own.shape[1]
    tops = []
    for at in blocks_of(half):
        total = dot(h_own[...], g_own[:, at], (1, 0)) + dot(h_peer[...], g_peer[:, at], (1, 0))
        out[:, at], top = code(total * scale)
        tops.append(top)
    out[:, half:] = tail_of(tops)


def start_kernel(core, q_t, out):
    half = out.shape[1]
    start = pl.multiple_of(core[0] * half, half)
    out[...] = nn(inverse_factor(nt(q_t[...], q_t[...])), q_t[:, pl.ds(start, half)])


def merge_kernel(core, terms, e_own, e_peer, own, peer, copies):
    rows, half = e_own.shape
    left = core[0] == 0
    for j, at in enumerate(blocks_of(half)):
        mine, other = e_own[:, at], e_peer[:, at]
        total = jnp.concatenate(
            [jnp.where(left, mine, other), jnp.where(left, other, mine)], axis=0
        )
        for source in range(terms.shape[0]):
            tail = terms[source, :, half:].astype(F32)
            total = total + decode(terms[source, :, at], tail[:, LANES * j : LANES * j + 1])
        own[:, at] = jnp.where(left, total[:rows], total[rows:])
        peer[:, at] = jnp.where(left, total[rows:], total[:rows])
        for target in range(copies.shape[0]):
            copies[target, :, at] = total


def sum_kernel(merged, copies):
    half = merged.shape[2]
    tops = []
    for at in blocks_of(half):
        coded, top = code(jnp.sum(merged[:, :, at], axis=0))
        tops.append(top)
        for target in range(copies.shape[0]):
            copies[target, :, at] = coded
    tail = tail_of(tops)
    for target in range(copies.shape[0]):
        copies[target, :, half:] = tail


def gram_kernel(q_t, coded, high, low, out):
    rank, half = q_t.shape
    rows = coded.shape[1]
    for pair in range(coded.shape[0] // 2):
        tails = [coded[2 * pair + k, :, half:].astype(F32) for k in range(2)]
        for j, at in enumerate(blocks_of(half)):
            values = [
                decode(coded[2 * pair + k, :, at], tails[k][:, LANES * j : LANES * j + 1])
                for k in range(2)
            ]
            to = pl.ds(2 * rows * pair, 2 * rows)
            high[to, at], low[to, at] = parts(jnp.concatenate(values, axis=0))
    summed = high[...], low[...]
    out[:rank, :] = dot3(parts(q_t[...]), summed, (1, 1))
    cross = dot(summed[0], summed[1], (1, 1))
    out[rank:, :] = dot(summed[0], summed[0], (1, 1)) + (cross + cross.T)


def power_kernel(own, peer, high_far, low_far, p_out, q_out, high, low, arrived):
    fetch = [
        pltpu.make_async_copy(high_far, high, arrived.at[0]),
        pltpu.make_async_copy(low_far, low, arrived.at[1]),
    ]
    for copy in fetch:
        copy.start()
    rank = p_out.shape[0]
    both = own[...] + peer[...]
    gram = both[rank:]
    p = orth_t(both[:rank])
    y = nn(p, gram)
    p = orth_t(nn(inverse_factor(nt(p, y)), y))
    p_out[...] = p
    for copy in fetch:
        copy.wait()
    q_out[...] = dot3(parts(p), (high[...], low[...]), (1, 0))


def last_kernel(n_rep, core, row, q_own, q_peer, p_t, m_own, m_peer, q_out, update, error):
    rows, half = m_peer.shape
    width = p_t.shape[1]
    want = row[0] + lax.broadcasted_iota(jnp.int32, (8, width), 0)
    pick = jnp.where(lax.broadcasted_iota(jnp.int32, (8, width), 1) == want, 1.0, 0.0)
    p_rows = nt(pick.astype(F32), p_t[...])
    left = core[0] == 0
    for side in range(2):
        at = pl.ds(side * half, half)
        mine = left if side == 0 else jnp.logical_not(left)
        q = jnp.where(mine, q_own[...], q_peer[...])
        merged = jnp.where(mine, m_own[...], m_peer[...])
        q_out[:, at] = q
        step = nn(p_rows, q)[:rows]
        update[:, at] = step
        error[:, at] = merged - step * (1.0 / n_rep)


def copies_kernel(own, copies):
    for target in range(copies.shape[0]):
        copies[target] = own[...]


def back_kernel(g, weight, out):
    out[...] = dot(g[...], weight[...], (1, 1))


def add_back_kernel(g, weight, other, out):
    out[...] = (dot(g[...], weight[...], (1, 1)) + other[...]).astype(BF16)


def swap(x):
    return lax.ppermute(x, CORE, [(0, 1), (1, 0)])


def side_of(x, side):
    half = x.shape[-1] // 2
    return lax.dynamic_slice_in_dim(x, side * half, half, x.ndim - 1)


def exchange(blocks, axes):
    return lax.all_to_all(blocks, axes, 0, 0, tiled=True)


def body(hidden, grad_out, weight_band, error_feedback, q_start):
    n_rep = lax.axis_size("rep")
    chips = lax.axis_size(CHIPS)
    tokens, units = hidden.shape
    scale = 1.0 / math.sqrt(tokens * lax.axis_size(SHARD) * n_rep)
    core = lax.axis_index(CORE)
    core_s = core.astype(jnp.int32)[None]
    row = (lax.axis_index(SHARD) * weight_band.shape[0]).astype(jnp.int32)[None]
    rows = weight_band.shape[0]
    half = grad_out.shape[1] // 2
    rank = q_start.shape[1]

    g_peer = swap(side_of(grad_out, 1 - core))
    h_own = hidden.T
    h_peer = swap(h_own)
    g_own = side_of(grad_out, core)
    terms = call(
        lambda *refs: partial_kernel(scale, *refs),
        far(units, half + TAIL, dtype=BF16),
        h_own,
        h_peer,
        g_own,
        g_peer,
    )
    terms = exchange(terms.reshape(chips, -1, half + TAIL), CHIPS)

    e_own = side_of(error_feedback[0], core)
    e_peer = swap(side_of(error_feedback[0], 1 - core))
    q_t = call(start_kernel, near(rank, half), core_s, q_start.T, scalars=1)
    w_own, w_peer = side_of(weight_band, core), swap(side_of(weight_band, 1 - core))
    weight = jnp.where(
        core == 0, jnp.concatenate([w_own, w_peer], 0), jnp.concatenate([w_peer, w_own], 0)
    )
    weight = call(copies_kernel, far(chips, *weight.shape, dtype=BF16), weight)
    terms, q_t, weight = lax.optimization_barrier((terms, q_t, weight))

    m_own, m_send, copies = call(
        merge_kernel,
        (near(rows, half), near(rows, half), near(n_rep, 2 * rows, half)),
        core_s,
        terms,
        e_own,
        e_peer,
        scalars=1,
    )
    copies = call(
        sum_kernel, far(chips, 2 * rows, half + TAIL, dtype=BF16), exchange(copies, "rep")
    )
    coded = exchange(copies, CHIPS)
    m_peer = swap(m_send)
    coded, m_peer = lax.optimization_barrier((coded, m_peer))
    high, low, grams = call(
        gram_kernel,
        (
            far(units, half, dtype=BF16),
            far(units, half, dtype=BF16),
            near(rank + units, units),
        ),
        q_t,
        coded,
    )
    grams, weight = lax.optimization_barrier((grams, weight))
    weight = exchange(weight, CHIPS).reshape(units, half)
    p_t, q_own = call(
        power_kernel,
        (near(rank, units), near(rank, half)),
        grams,
        swap(grams),
        high,
        low,
        held=(2, 3),
        scratch=(
            pltpu.VMEM((units, half), BF16),
            pltpu.VMEM((units, half), BF16),
            pltpu.SemaphoreType.DMA((2,)),
        ),
    )
    q_next, update, error = call(
        lambda *refs: last_kernel(n_rep, *refs),
        (far(rank, 2 * half), far(rows, 2 * half), far(rows, 2 * half)),
        core_s,
        row,
        q_own,
        swap(q_own),
        p_t,
        m_own,
        m_peer,
        scalars=2,
    )
    weight, q_next = lax.optimization_barrier((weight, q_next))
    d_send = call(back_kernel, near(tokens, units), g_peer, weight)
    d_hidden = call(
        add_back_kernel, far(tokens, units, dtype=BF16), g_own, weight, swap(d_send)
    )
    return (update, error[None], q_next.T, d_hidden)


def solution(mesh):
    finer = Mesh(
        mesh.devices.reshape(mesh.shape["rep"], 4, 8, 2), ("rep", "shard_0", "shard_1", "shard_2")
    )
    placed = (P(REP_SHARD, None), P(REP_SHARD, None), P(SHARD, None), P("rep", SHARD, None), P())
    return jax.shard_map(
        body,
        mesh=finer,
        in_specs=placed,
        out_specs=(P(SHARD, None), P("rep", SHARD, None), P(), P(REP_SHARD, None)),
        check_vma=False,
    )
```

```python
import math

import jax
import jax.numpy as jnp
from jax import lax
from jax.experimental import pallas as pl
from jax.experimental.pallas import tpu as pltpu
from jax.sharding import Mesh
from jax.sharding import PartitionSpec as P

SHARD = ("shard_0", "shard_1", "shard_2")
REP_SHARD = ("rep", "shard_0", "shard_1", "shard_2")
CHIPS = ("shard_0", "shard_1")
CORE = "shard_2"
HIGHEST = lax.Precision.HIGHEST
F32, BF16 = jnp.float32, jnp.bfloat16
SPAN = 250.0
LN2 = math.log(2.0)
BLOCK = 512
TAIL = 128
LANES = 32
PANEL = 8


def dot(a, b, over, precision=None):
    return lax.dot_general(
        a, b, ((over[:1], over[1:]), ((), ())), precision=precision, preferred_element_type=F32
    )


def nn(a, b):
    return dot(a, b, (1, 0), HIGHEST)


def nt(a, b):
    return dot(a, b, (1, 1), HIGHEST)


def parts(x):
    high = x.astype(BF16)
    return high, (x - high.astype(F32)).astype(BF16)


def dot3(a, b, over):
    return dot(a[0], b[0], over) + (dot(a[0], b[1], over) + dot(a[1], b[0], over))


def inverse_factor(gram):
    n = gram.shape[0]
    rows = lax.broadcasted_iota(jnp.int32, (n, n), 0)
    cols = lax.broadcasted_iota(jnp.int32, (n, n), 1)
    a, b = gram, jnp.where(rows == cols, 1.0, 0.0).astype(F32)
    for j in range(0, n, PANEL):
        tall = [jnp.broadcast_to(a[:, j + m : j + m + 1], (n, n)) for m in range(PANEL)]
        left = [a[j + m : j + m + 1, :] for m in range(PANEL)]
        right = [b[j + m : j + m + 1, :] for m in range(PANEL)]
        for m in range(PANEL):
            at = j + m
            tall[m] = jnp.where(rows > at, tall[m] * (1.0 / tall[m][at : at + 1, :]), 0.0)
            for k in range(m + 1, PANEL):
                tall[k] = tall[k] - tall[m] * tall[k][at : at + 1, :]
                factor = tall[m][j + k : j + k + 1, :]
                left[k], right[k] = left[k] - factor * left[m], right[k] - factor * right[m]
        for m in range(PANEL):
            a, b = a - tall[m] * left[m], b - tall[m] * right[m]
    pivots = jnp.sum(jnp.where(rows == cols, a, 0.0), axis=1, keepdims=True)
    return b * (1.0 / jnp.sqrt(pivots))


def orth_t(x):
    return nn(inverse_factor(nt(x, x)), x)


def code(x):
    top = jnp.max(jnp.abs(x), axis=1, keepdims=True)
    top = jnp.maximum(top * 1.01, 1e-30).astype(BF16).astype(F32)
    level = jnp.sqrt(jnp.abs(x) * (1.0 / top))
    size = jnp.exp(level * (SPAN * LN2) - (SPAN * LN2 / 2))
    return jnp.where(x < 0, -size, size).astype(BF16), top


def decode(y, top):
    y = y.astype(F32)
    level = jnp.log(jnp.abs(y)) * (1.0 / (SPAN * LN2)) + 0.5
    size = level * level * top
    return jnp.where(y < 0, -size, size)


def tail_of(tops):
    wide = [jnp.broadcast_to(top, (top.shape[0], LANES)) for top in tops]
    return jnp.concatenate(wide, axis=1).astype(BF16)


def blocks_of(half):
    return [pl.ds(j * BLOCK, BLOCK) for j in range(half // BLOCK)]


def near(*shape, dtype=F32):
    return pltpu.VMEM(shape, dtype)


def far(*shape, dtype=F32):
    return jax.ShapeDtypeStruct(shape, dtype)


def call(kernel, out, *args, scalars=0, held=(), kept=(), scratch=()):
    vmem = pl.BlockSpec(memory_space=pltpu.VMEM)
    smem = pl.BlockSpec(memory_space=pltpu.SMEM)
    hbm = pl.BlockSpec(memory_space=pltpu.HBM)
    kinds = [smem if i < scalars else hbm if i in held else vmem for i in range(len(args))]
    placed = [
        x if kind is smem else pltpu.with_memory_space_constraint(x, kind.memory_space)
        for x, kind in zip(args, kinds)
    ]
    return pl.pallas_call(
        kernel,
        out_shape=out,
        in_specs=kinds,
        out_specs=tuple(hbm if i in kept else vmem for i in range(len(out)))
        if isinstance(out, tuple)
        else vmem,
        scratch_shapes=list(scratch),
        compiler_params=pltpu.CompilerParams(vmem_limit_bytes=24 << 20),
    )(*placed)


def fetched(far, start, held, arrived):
    copies = []
    for j, at in enumerate(blocks_of(held.shape[1])):
        columns = pl.ds(pl.multiple_of(start + j * BLOCK, BLOCK), BLOCK)
        copies.append(pltpu.make_async_copy(far.at[:, columns], held.at[:, at], arrived.at[j]))
        copies[-1].start()
    return copies


def side_kernel(core, g_far, out, arrived):
    half = out.shape[1]
    for copy in fetched(g_far, (1 - core[0]) * half, out, arrived):
        copy.wait()


def partial_kernel(scale, core, h_own, h_peer, g_far, g_peer, out, g_own, arrived):
    half = g_own.shape[1]
    copies = fetched(g_far, core[0] * half, g_own, arrived)
    tops = []
    for copy, at in zip(copies, blocks_of(half)):
        total = dot(h_peer[...], g_peer[:, at], (1, 0))
        copy.wait()
        total = total + dot(h_own[...], g_own[:, at], (1, 0))
        out[:, at], top = code(total * scale)
        tops.append(top)
    out[:, half:] = tail_of(tops)


def start_kernel(core, q_t, out):
    half = out.shape[1]
    start = pl.multiple_of(core[0] * half, half)
    out[...] = nn(inverse_factor(nt(q_t[...], q_t[...])), q_t[:, pl.ds(start, half)])


def merge_kernel(core, terms, e_own, e_peer, own, peer, copies):
    rows, half = e_own.shape
    left = core[0] == 0
    for j, at in enumerate(blocks_of(half)):
        mine, other = e_own[:, at], e_peer[:, at]
        total = jnp.concatenate(
            [jnp.where(left, mine, other), jnp.where(left, other, mine)], axis=0
        )
        for source in range(terms.shape[0]):
            tail = terms[source, :, half:].astype(F32)
            total = total + decode(terms[source, :, at], tail[:, LANES * j : LANES * j + 1])
        own[:, at] = jnp.where(left, total[:rows], total[rows:])
        peer[:, at] = jnp.where(left, total[rows:], total[:rows])
        for target in range(copies.shape[0]):
            copies[target, :, at] = total


def sum_kernel(merged, copies):
    half = merged.shape[2]
    tops = []
    for at in blocks_of(half):
        coded, top = code(jnp.sum(merged[:, :, at], axis=0))
        tops.append(top)
        for target in range(copies.shape[0]):
            copies[target, :, at] = coded
    tail = tail_of(tops)
    for target in range(copies.shape[0]):
        copies[target, :, half:] = tail


def gram_kernel(q_t, coded, high_far, low_far, out, high, low, sent):
    rank, half = q_t.shape
    rows = coded.shape[1]
    for pair in range(coded.shape[0] // 2):
        tails = [coded[2 * pair + k, :, half:].astype(F32) for k in range(2)]
        for j, at in enumerate(blocks_of(half)):
            values = [
                decode(coded[2 * pair + k, :, at], tails[k][:, LANES * j : LANES * j + 1])
                for k in range(2)
            ]
            to = pl.ds(2 * rows * pair, 2 * rows)
            high[to, at], low[to, at] = parts(jnp.concatenate(values, axis=0))
    store = [
        pltpu.make_async_copy(high, high_far, sent.at[0]),
        pltpu.make_async_copy(low, low_far, sent.at[1]),
    ]
    for copy in store:
        copy.start()
    summed = high[...], low[...]
    out[:rank, :] = dot3(parts(q_t[...]), summed, (1, 1))
    cross = dot(summed[0], summed[1], (1, 1))
    out[rank:, :] = dot(summed[0], summed[0], (1, 1)) + (cross + cross.T)
    for copy in store:
        copy.wait()


def power_kernel(own, peer, high_far, low_far, p_out, q_out, high, low, arrived):
    fetch = [
        pltpu.make_async_copy(high_far, high, arrived.at[0]),
        pltpu.make_async_copy(low_far, low, arrived.at[1]),
    ]
    for copy in fetch:
        copy.start()
    rank = p_out.shape[0]
    both = own[...] + peer[...]
    gram = both[rank:]
    p = orth_t(both[:rank])
    y = nn(p, gram)
    p = orth_t(nn(inverse_factor(nt(p, y)), y))
    p_out[...] = p
    for copy in fetch:
        copy.wait()
    q_out[...] = dot3(parts(p), (high[...], low[...]), (1, 0))


def last_kernel(n_rep, core, row, q_own, q_peer, p_t, m_own, m_peer, q_out, update, error):
    rows, half = m_peer.shape
    width = p_t.shape[1]
    want = row[0] + lax.broadcasted_iota(jnp.int32, (8, width), 0)
    pick = jnp.where(lax.broadcasted_iota(jnp.int32, (8, width), 1) == want, 1.0, 0.0)
    p_rows = nt(pick.astype(F32), p_t[...])
    left = core[0] == 0
    for side in range(2):
        at = pl.ds(side * half, half)
        mine = left if side == 0 else jnp.logical_not(left)
        q = jnp.where(mine, q_own[...], q_peer[...])
        merged = jnp.where(mine, m_own[...], m_peer[...])
        q_out[:, at] = q
        step = nn(p_rows, q)[:rows]
        update[:, at] = step
        error[:, at] = merged - step * (1.0 / n_rep)


def copies_kernel(own, copies):
    for target in range(copies.shape[0]):
        copies[target] = own[...]


def product_with(weight, copies, held):
    total = 0.0
    for copy, at in zip(copies, blocks_of(held.shape[1])):
        copy.wait()
        total = total + dot(held[:, at], weight[:, at], (1, 1))
    return total


def back_kernel(weight, g_far, out, held, arrived):
    out[...] = product_with(weight, fetched(g_far, 0, held, arrived), held)


def add_back_kernel(core, weight, other, g_far, out, held, arrived):
    copies = fetched(g_far, core[0] * held.shape[1], held, arrived)
    out[...] = (product_with(weight, copies, held) + other[...]).astype(BF16)


def swap(x):
    return lax.ppermute(x, CORE, [(0, 1), (1, 0)])


def side_of(x, side):
    half = x.shape[-1] // 2
    return lax.dynamic_slice_in_dim(x, side * half, half, x.ndim - 1)


def exchange(blocks, axes):
    return lax.all_to_all(blocks, axes, 0, 0, tiled=True)


def step(hidden, grad_out, weight_band, error_feedback, q_start):
    n_rep = lax.axis_size("rep")
    chips = lax.axis_size(CHIPS)
    tokens, units = hidden.shape
    scale = 1.0 / math.sqrt(tokens * lax.axis_size(SHARD) * n_rep)
    core = lax.axis_index(CORE)
    core_s = core.astype(jnp.int32)[None]
    row = (lax.axis_index(SHARD) * weight_band.shape[0]).astype(jnp.int32)[None]
    rows = weight_band.shape[0]
    half = grad_out.shape[1] // 2
    rank = q_start.shape[1]

    blocks = pltpu.SemaphoreType.DMA((half // BLOCK,))
    side = (pltpu.VMEM((tokens, half), BF16), blocks)
    g_send = call(
        side_kernel,
        near(tokens, half, dtype=BF16),
        core_s,
        grad_out,
        scalars=1,
        held=(1,),
        scratch=(blocks,),
    )
    g_peer = swap(g_send)
    h_own = hidden.T
    h_peer = swap(h_own)
    terms = call(
        lambda *refs: partial_kernel(scale, *refs),
        far(units, half + TAIL, dtype=BF16),
        core_s,
        h_own,
        h_peer,
        grad_out,
        g_peer,
        scalars=1,
        held=(3,),
        scratch=side,
    )
    terms = exchange(terms.reshape(chips, -1, half + TAIL), CHIPS)

    e_own = side_of(error_feedback[0], core)
    e_peer = swap(side_of(error_feedback[0], 1 - core))
    q_t = call(start_kernel, near(rank, half), core_s, q_start.T, scalars=1)
    w_own, w_peer = side_of(weight_band, core), swap(side_of(weight_band, 1 - core))
    weight = jnp.where(
        core == 0, jnp.concatenate([w_own, w_peer], 0), jnp.concatenate([w_peer, w_own], 0)
    )
    weight = call(copies_kernel, far(chips, *weight.shape, dtype=BF16), weight)
    terms, q_t, weight = lax.optimization_barrier((terms, q_t, weight))

    m_own, m_send, copies = call(
        merge_kernel,
        (near(rows, half), near(rows, half), near(n_rep, 2 * rows, half)),
        core_s,
        terms,
        e_own,
        e_peer,
        scalars=1,
    )
    copies = call(
        sum_kernel, far(chips, 2 * rows, half + TAIL, dtype=BF16), exchange(copies, "rep")
    )
    coded = exchange(copies, CHIPS)
    m_peer = swap(m_send)
    coded, m_peer = lax.optimization_barrier((coded, m_peer))
    pieces = (
        pltpu.VMEM((units, half), BF16),
        pltpu.VMEM((units, half), BF16),
        pltpu.SemaphoreType.DMA((2,)),
    )
    high, low, grams = call(
        gram_kernel,
        (
            pltpu.HBM((units, half), BF16),
            pltpu.HBM((units, half), BF16),
            near(rank + units, units),
        ),
        q_t,
        coded,
        kept=(0, 1),
        scratch=pieces,
    )
    grams, weight = lax.optimization_barrier((grams, weight))
    weight = exchange(weight, CHIPS)
    weight = weight.reshape(units, half)
    other = swap(grams)
    p_t, q_own = call(
        power_kernel,
        (near(rank, units), near(rank, half)),
        grams,
        other,
        high,
        low,
        held=(2, 3),
        scratch=pieces,
    )
    q_other = swap(q_own)
    weight, p_t = lax.optimization_barrier((weight, p_t))
    q_next, update, error = call(
        lambda *refs: last_kernel(n_rep, *refs),
        (far(rank, 2 * half), far(rows, 2 * half), far(rows, 2 * half)),
        core_s,
        row,
        q_own,
        q_other,
        p_t,
        m_own,
        m_peer,
        scalars=2,
    )
    d_send = call(back_kernel, near(tokens, units), weight, g_peer, held=(1,), scratch=side)
    d_other = swap(d_send)
    d_hidden = call(
        add_back_kernel,
        far(tokens, units, dtype=BF16),
        core_s,
        weight,
        d_other,
        grad_out,
        scalars=1,
        held=(3,),
        scratch=side,
    )
    return (update, error[None], q_next.T, d_hidden)


def solution(mesh):
    finer = Mesh(
        mesh.devices.reshape(mesh.shape["rep"], 4, 8, 2), ("rep", "shard_0", "shard_1", "shard_2")
    )
    placed = (P(REP_SHARD, None), P(REP_SHARD, None), P(SHARD, None), P("rep", SHARD, None), P())
    return jax.shard_map(
        step,
        mesh=finer,
        in_specs=placed,
        out_specs=(P(SHARD, None), P("rep", SHARD, None), P(), P(REP_SHARD, None)),
        check_vma=False,
    )
```

```python
import math

import jax
import jax.numpy as jnp
from jax import lax
from jax.experimental import pallas as pl
from jax.experimental.pallas import tpu as pltpu
from jax.sharding import Mesh
from jax.sharding import PartitionSpec as P

SHARD = ("shard_0", "shard_1", "shard_2")
REP_SHARD = ("rep", "shard_0", "shard_1", "shard_2")
CHIPS = ("shard_0", "shard_1")
CORE = "shard_2"
HIGHEST = lax.Precision.HIGHEST
F32, BF16 = jnp.float32, jnp.bfloat16
SPAN = 250.0
LN2 = math.log(2.0)
BLOCK = 512
TAIL = 128
LANES = 32
PANEL = 8
PIECE = 256


def dot(a, b, over, precision=None):
    return lax.dot_general(
        a, b, ((over[:1], over[1:]), ((), ())), precision=precision, preferred_element_type=F32
    )


def nn(a, b):
    return dot(a, b, (1, 0), HIGHEST)


def nt(a, b):
    return dot(a, b, (1, 1), HIGHEST)


def parts(x):
    high = x.astype(BF16)
    return high, (x - high.astype(F32)).astype(BF16)


def dot3(a, b, over):
    return dot(a[0], b[0], over) + (dot(a[0], b[1], over) + dot(a[1], b[0], over))


def inverse_factor(gram):
    n = gram.shape[0]
    rows = lax.broadcasted_iota(jnp.int32, (n, n), 0)
    cols = lax.broadcasted_iota(jnp.int32, (n, n), 1)
    a, b = gram, jnp.where(rows == cols, 1.0, 0.0).astype(F32)
    for j in range(0, n, PANEL):
        tall = [jnp.broadcast_to(a[:, j + m : j + m + 1], (n, n)) for m in range(PANEL)]
        left = [a[j + m : j + m + 1, :] for m in range(PANEL)]
        right = [b[j + m : j + m + 1, :] for m in range(PANEL)]
        for m in range(PANEL):
            at = j + m
            tall[m] = jnp.where(rows > at, tall[m] * (1.0 / tall[m][at : at + 1, :]), 0.0)
            for k in range(m + 1, PANEL):
                tall[k] = tall[k] - tall[m] * tall[k][at : at + 1, :]
                factor = tall[m][j + k : j + k + 1, :]
                left[k], right[k] = left[k] - factor * left[m], right[k] - factor * right[m]
        for m in range(PANEL):
            a, b = a - tall[m] * left[m], b - tall[m] * right[m]
    pivots = jnp.sum(jnp.where(rows == cols, a, 0.0), axis=1, keepdims=True)
    return b * (1.0 / jnp.sqrt(pivots))


def orth_t(x):
    return nn(inverse_factor(nt(x, x)), x)


def code(x):
    top = jnp.max(jnp.abs(x), axis=1, keepdims=True)
    top = jnp.maximum(top * 1.01, 1e-30).astype(BF16).astype(F32)
    level = jnp.sqrt(jnp.abs(x) * (1.0 / top))
    size = jnp.exp(level * (SPAN * LN2) - (SPAN * LN2 / 2))
    return jnp.where(x < 0, -size, size).astype(BF16), top


def decode(y, top):
    y = y.astype(F32)
    level = jnp.log(jnp.abs(y)) * (1.0 / (SPAN * LN2)) + 0.5
    size = level * level * top
    return jnp.where(y < 0, -size, size)


def tail_of(tops):
    wide = [jnp.broadcast_to(top, (top.shape[0], LANES)) for top in tops]
    return jnp.concatenate(wide, axis=1).astype(BF16)


def blocks_of(half):
    return [pl.ds(j * BLOCK, BLOCK) for j in range(half // BLOCK)]


def near(*shape, dtype=F32):
    return pltpu.VMEM(shape, dtype)


def far(*shape, dtype=F32):
    return jax.ShapeDtypeStruct(shape, dtype)


def call(kernel, out, *args, scalars=0, held=(), kept=(), scratch=()):
    vmem = pl.BlockSpec(memory_space=pltpu.VMEM)
    smem = pl.BlockSpec(memory_space=pltpu.SMEM)
    hbm = pl.BlockSpec(memory_space=pltpu.HBM)
    kinds = [smem if i < scalars else hbm if i in held else vmem for i in range(len(args))]
    placed = [
        x if kind is smem else pltpu.with_memory_space_constraint(x, kind.memory_space)
        for x, kind in zip(args, kinds)
    ]
    return pl.pallas_call(
        kernel,
        out_shape=out,
        in_specs=kinds,
        out_specs=tuple(hbm if i in kept else vmem for i in range(len(out)))
        if isinstance(out, tuple)
        else vmem,
        scratch_shapes=list(scratch),
        compiler_params=pltpu.CompilerParams(vmem_limit_bytes=24 << 20),
    )(*placed)


def fetched(far, start, held, arrived):
    copies = []
    for j, at in enumerate(blocks_of(held.shape[1])):
        columns = pl.ds(pl.multiple_of(start + j * BLOCK, BLOCK), BLOCK)
        copies.append(pltpu.make_async_copy(far.at[:, columns], held.at[:, at], arrived.at[j]))
        copies[-1].start()
    return copies


def side_kernel(core, g_far, out, arrived):
    half = out.shape[1]
    for copy in fetched(g_far, (1 - core[0]) * half, out, arrived):
        copy.wait()


def partial_kernel(scale, core, rep, h_own, h_peer, weight, g_far, g_peer, out, g_own, arrived):
    half = g_own.shape[1]
    copies = fetched(g_far, core[0] * half, g_own, arrived)
    start = rep[0] * PIECE
    sides = [
        weight[:, pl.ds(pl.multiple_of(side * half + start, PIECE), PIECE)].astype(F32)
        for side in range(2)
    ]
    piece = jnp.concatenate(sides + sides, axis=0).astype(BF16)
    for at in range(0, out.shape[0], piece.shape[0]):
        out[at : at + piece.shape[0], half + TAIL :] = piece
    tops = []
    for copy, at in zip(copies, blocks_of(half)):
        total = dot(h_peer[...], g_peer[:, at], (1, 0))
        copy.wait()
        total = total + dot(h_own[...], g_own[:, at], (1, 0))
        out[:, at], top = code(total * scale)
        tops.append(top)
    out[:, half : half + TAIL] = tail_of(tops)


def start_kernel(core, q_t, out):
    half = out.shape[1]
    start = pl.multiple_of(core[0] * half, half)
    out[...] = nn(inverse_factor(nt(q_t[...], q_t[...])), q_t[:, pl.ds(start, half)])


def tail_at(terms, half):
    return terms[:, half : half + TAIL].astype(F32)


def merge_kernel(core, terms, e_own, e_peer, own, peer, copies):
    rows, half = e_own.shape
    n_rep = copies.shape[0]
    left = core[0] == 0
    tops = []
    for j, at in enumerate(blocks_of(half)):
        mine, other = e_own[:, at], e_peer[:, at]
        total = jnp.concatenate(
            [jnp.where(left, mine, other), jnp.where(left, other, mine)], axis=0
        )
        for source in range(terms.shape[0]):
            tail = tail_at(terms[source], half)
            total = total + decode(terms[source, :, at], tail[:, LANES * j : LANES * j + 1])
        own[:, at] = jnp.where(left, total[:rows], total[rows:])
        peer[:, at] = jnp.where(left, total[rows:], total[:rows])
        coded, top = code(total)
        tops.append(top)
        for target in range(n_rep):
            copies[target, 0, :, at] = coded
    tail = tail_of(tops)
    across = half // PIECE
    for target in range(n_rep):
        for group in range(copies.shape[1]):
            copies[target, group, :, half:] = tail
        for source in range(terms.shape[0]):
            to = pl.ds(source % across * PIECE, PIECE)
            copies[target, 1 + source // across, :, to] = terms[source, :, half + TAIL :]


def sum_kernel(merged, copies):
    half = copies.shape[2] - TAIL
    tops = []
    for j, at in enumerate(blocks_of(half)):
        total = 0.0
        for source in range(merged.shape[0]):
            tail = tail_at(merged[source, 0], half)
            total = total + decode(merged[source, 0, :, at], tail[:, LANES * j : LANES * j + 1])
        coded, top = code(total)
        tops.append(top)
        for target in range(copies.shape[0]):
            copies[target, :, at] = coded
    tail = tail_of(tops)
    for target in range(copies.shape[0]):
        copies[target, :, half:] = tail


def weight_kernel(merged, out):
    across = out.shape[2] // PIECE
    for source in range(merged.shape[0]):
        to = pl.ds(source * PIECE, PIECE)
        for chip in range(out.shape[0]):
            at = pl.ds(chip % across * PIECE, PIECE)
            out[chip, :, to] = merged[source, 1 + chip // across, :, at]


def hidden_kernel(rows, core, w_own, w_peer, g_far, out, g, arrived):
    half = w_own.shape[1]
    copies = fetched(g_far, 0, g, arrived)
    sums = [[0.0, 0.0], [0.0, 0.0]]
    for j, (copy, at) in enumerate(zip(copies, blocks_of(2 * half))):
        copy.wait()
        side = j * BLOCK // half
        columns = pl.ds(j * BLOCK % half, BLOCK)
        for which, weight in enumerate((w_own, w_peer)):
            sums[which][side] = sums[which][side] + dot(g[:, at], weight[:, columns], (1, 1))
    lane = lax.broadcasted_iota(jnp.int32, out.shape, 1)
    first = lane // rows % 2 == 0
    whole = []
    for which in range(2):
        term = jnp.where(first, sums[which][0], sums[which][1])
        width = term.shape[1]
        other = jnp.where(
            first, pltpu.roll(term, width - rows, 1), pltpu.roll(term, rows, 1)
        )
        whole.append(term + other)
    out[...] = jnp.where(first == (core[0] == 0), whole[0], whole[1]).astype(BF16)


def gram_kernel(q_t, coded, high_far, low_far, out, high, low, sent):
    rank, half = q_t.shape
    rows = coded.shape[1]
    for pair in range(coded.shape[0] // 2):
        tails = [coded[2 * pair + k, :, half:].astype(F32) for k in range(2)]
        for j, at in enumerate(blocks_of(half)):
            values = [
                decode(coded[2 * pair + k, :, at], tails[k][:, LANES * j : LANES * j + 1])
                for k in range(2)
            ]
            to = pl.ds(2 * rows * pair, 2 * rows)
            high[to, at], low[to, at] = parts(jnp.concatenate(values, axis=0))
    store = [
        pltpu.make_async_copy(high, high_far, sent.at[0]),
        pltpu.make_async_copy(low, low_far, sent.at[1]),
    ]
    for copy in store:
        copy.start()
    summed = high[...], low[...]
    out[:rank, :] = dot3(parts(q_t[...]), summed, (1, 1))
    cross = dot(summed[0], summed[1], (1, 1))
    out[rank:, :] = dot(summed[0], summed[0], (1, 1)) + (cross + cross.T)
    for copy in store:
        copy.wait()


def power_kernel(own, peer, high_far, low_far, p_out, q_out, high, low, arrived):
    fetch = [
        pltpu.make_async_copy(high_far, high, arrived.at[0]),
        pltpu.make_async_copy(low_far, low, arrived.at[1]),
    ]
    for copy in fetch:
        copy.start()
    rank = p_out.shape[0]
    both = own[...] + peer[...]
    gram = both[rank:]
    p = orth_t(both[:rank])
    y = nn(p, gram)
    p = orth_t(nn(inverse_factor(nt(p, y)), y))
    p_out[...] = p
    for copy in fetch:
        copy.wait()
    q_out[...] = dot3(parts(p), (high[...], low[...]), (1, 0))


def last_kernel(n_rep, core, row, q_own, q_peer, p_t, m_own, m_peer, q_out, update, error):
    rows, half = m_peer.shape
    width = p_t.shape[1]
    want = row[0] + lax.broadcasted_iota(jnp.int32, (8, width), 0)
    pick = jnp.where(lax.broadcasted_iota(jnp.int32, (8, width), 1) == want, 1.0, 0.0)
    p_rows = nt(pick.astype(F32), p_t[...])
    left = core[0] == 0
    for side in range(2):
        at = pl.ds(side * half, half)
        mine = left if side == 0 else jnp.logical_not(left)
        q = jnp.where(mine, q_own[...], q_peer[...])
        merged = jnp.where(mine, m_own[...], m_peer[...])
        q_out[:, at] = q
        step = nn(p_rows, q)[:rows]
        update[:, at] = step
        error[:, at] = merged - step * (1.0 / n_rep)


def swap(x):
    return lax.ppermute(x, CORE, [(0, 1), (1, 0)])


def side_of(x, side):
    half = x.shape[-1] // 2
    return lax.dynamic_slice_in_dim(x, side * half, half, x.ndim - 1)


def exchange(blocks, axes):
    return lax.all_to_all(blocks, axes, 0, 0, tiled=True)


def body(hidden, grad_out, weight_band, error_feedback, q_start):
    n_rep = lax.axis_size("rep")
    chips = lax.axis_size(CHIPS)
    tokens, units = hidden.shape
    scale = 1.0 / math.sqrt(tokens * lax.axis_size(SHARD) * n_rep)
    core = lax.axis_index(CORE)
    core_s = core.astype(jnp.int32)[None]
    row = (lax.axis_index(SHARD) * weight_band.shape[0]).astype(jnp.int32)[None]
    rows = weight_band.shape[0]
    half = grad_out.shape[1] // 2
    rank = q_start.shape[1]

    blocks = pltpu.SemaphoreType.DMA((half // BLOCK,))
    g_send = call(
        side_kernel,
        near(tokens, half, dtype=BF16),
        core_s,
        grad_out,
        scalars=1,
        held=(1,),
        scratch=(blocks,),
    )
    g_peer = swap(g_send)
    h_own = hidden.T
    h_peer = swap(h_own)
    terms = call(
        lambda *refs: partial_kernel(scale, *refs),
        far(units, half + TAIL + PIECE, dtype=BF16),
        core_s,
        lax.axis_index("rep").astype(jnp.int32)[None],
        h_own,
        h_peer,
        weight_band,
        grad_out,
        g_peer,
        scalars=2,
        held=(5,),
        scratch=(pltpu.VMEM((tokens, half), BF16), blocks),
    )
    terms = exchange(terms.reshape(chips, 2 * rows, -1), CHIPS)

    e_own = side_of(error_feedback[0], core)
    e_peer = swap(side_of(error_feedback[0], 1 - core))
    q_t = call(start_kernel, near(rank, half), core_s, q_start.T, scalars=1)
    terms, q_t = lax.optimization_barrier((terms, q_t))

    m_own, m_send, copies = call(
        merge_kernel,
        (
            near(rows, half),
            near(rows, half),
            near(n_rep, 1 + chips * PIECE // half, 2 * rows, half + TAIL, dtype=BF16),
        ),
        core_s,
        terms,
        e_own,
        e_peer,
        scalars=1,
    )
    merged = exchange(copies, "rep")
    copies = call(sum_kernel, far(chips, 2 * rows, half + TAIL, dtype=BF16), merged)
    coded = exchange(copies, CHIPS)

    w_own = call(weight_kernel, near(chips, 2 * rows, half, dtype=BF16), merged)
    w_own = w_own.reshape(units, half)
    d_hidden = call(
        lambda *refs: hidden_kernel(rows, *refs),
        far(tokens, units, dtype=BF16),
        core_s,
        w_own,
        swap(w_own),
        grad_out,
        scalars=1,
        held=(3,),
        scratch=(
            pltpu.VMEM((tokens, 2 * half), BF16),
            pltpu.SemaphoreType.DMA((2 * half // BLOCK,)),
        ),
    )
    m_peer = swap(m_send)
    coded, m_peer, d_hidden = lax.optimization_barrier((coded, m_peer, d_hidden))
    pieces = (
        pltpu.VMEM((units, half), BF16),
        pltpu.VMEM((units, half), BF16),
        pltpu.SemaphoreType.DMA((2,)),
    )
    high, low, grams = call(
        gram_kernel,
        (
            pltpu.HBM((units, half), BF16),
            pltpu.HBM((units, half), BF16),
            near(rank + units, units),
        ),
        q_t,
        coded,
        kept=(0, 1),
        scratch=pieces,
    )
    p_t, q_own = call(
        power_kernel,
        (near(rank, units), near(rank, half)),
        grams,
        swap(grams),
        high,
        low,
        held=(2, 3),
        scratch=pieces,
    )
    q_next, update, error = call(
        lambda *refs: last_kernel(n_rep, *refs),
        (far(rank, 2 * half), far(rows, 2 * half), far(rows, 2 * half)),
        core_s,
        row,
        q_own,
        swap(q_own),
        p_t,
        m_own,
        m_peer,
        scalars=2,
    )
    return (update, error[None], q_next.T, d_hidden)


def solution(mesh):
    finer = Mesh(
        mesh.devices.reshape(mesh.shape["rep"], 4, 8, 2), ("rep", "shard_0", "shard_1", "shard_2")
    )
    placed = (P(REP_SHARD, None), P(REP_SHARD, None), P(SHARD, None), P("rep", SHARD, None), P())
    return jax.shard_map(
        body,
        mesh=finer,
        in_specs=placed,
        out_specs=(P(SHARD, None), P("rep", SHARD, None), P(), P(REP_SHARD, None)),
        check_vma=False,
    )
```

```python
import math

import jax
import jax.numpy as jnp
from jax import lax
from jax.experimental import pallas as pl
from jax.experimental.pallas import tpu as pltpu
from jax.sharding import Mesh
from jax.sharding import PartitionSpec as P

SHARD = ("shard_0", "shard_1", "shard_2")
REP = ("rep_0", "rep_1")
REP_SHARD = REP + SHARD
CHIPS = ("shard_0", "shard_1")
CORE = "shard_2"
HIGHEST = lax.Precision.HIGHEST
F32, BF16 = jnp.float32, jnp.bfloat16
SPAN = 250.0
LN2 = math.log(2.0)
BLOCK = 512
TAIL = 128
LANES = 32
PANEL = 8
PIECE = 512


def dot(a, b, over, precision=None):
    return lax.dot_general(
        a, b, ((over[:1], over[1:]), ((), ())), precision=precision, preferred_element_type=F32
    )


def nn(a, b):
    return dot(a, b, (1, 0), HIGHEST)


def nt(a, b):
    return dot(a, b, (1, 1), HIGHEST)


def parts(x):
    high = x.astype(BF16)
    return high, (x - high.astype(F32)).astype(BF16)


def dot3(a, b, over):
    return dot(a[0], b[0], over) + (dot(a[0], b[1], over) + dot(a[1], b[0], over))


def inverse_factor(gram):
    n = gram.shape[0]
    rows = lax.broadcasted_iota(jnp.int32, (n, n), 0)
    cols = lax.broadcasted_iota(jnp.int32, (n, n), 1)
    a, b = gram, jnp.where(rows == cols, 1.0, 0.0).astype(F32)
    for j in range(0, n, PANEL):
        tall = [jnp.broadcast_to(a[:, j + m : j + m + 1], (n, n)) for m in range(PANEL)]
        left = [a[j + m : j + m + 1, :] for m in range(PANEL)]
        right = [b[j + m : j + m + 1, :] for m in range(PANEL)]
        for m in range(PANEL):
            at = j + m
            tall[m] = jnp.where(rows > at, tall[m] * (1.0 / tall[m][at : at + 1, :]), 0.0)
            for k in range(m + 1, PANEL):
                tall[k] = tall[k] - tall[m] * tall[k][at : at + 1, :]
                factor = tall[m][j + k : j + k + 1, :]
                left[k], right[k] = left[k] - factor * left[m], right[k] - factor * right[m]
        for m in range(PANEL):
            a, b = a - tall[m] * left[m], b - tall[m] * right[m]
    pivots = jnp.sum(jnp.where(rows == cols, a, 0.0), axis=1, keepdims=True)
    return b * (1.0 / jnp.sqrt(pivots))


def orth_t(x):
    return nn(inverse_factor(nt(x, x)), x)


def code(x):
    top = jnp.max(jnp.abs(x), axis=1, keepdims=True)
    top = jnp.maximum(top * 1.01, 1e-30).astype(BF16).astype(F32)
    level = jnp.sqrt(jnp.abs(x) * (1.0 / top))
    size = jnp.exp(level * (SPAN * LN2) - (SPAN * LN2 / 2))
    return jnp.where(x < 0, -size, size).astype(BF16), top


def decode(y, top):
    y = y.astype(F32)
    level = jnp.log(jnp.abs(y)) * (1.0 / (SPAN * LN2)) + 0.5
    size = level * level * top
    return jnp.where(y < 0, -size, size)


def tail_of(tops):
    wide = [jnp.broadcast_to(top, (top.shape[0], LANES)) for top in tops]
    return jnp.concatenate(wide, axis=1).astype(BF16)


def blocks_of(half):
    return [pl.ds(j * BLOCK, BLOCK) for j in range(half // BLOCK)]


def near(*shape, dtype=F32):
    return pltpu.VMEM(shape, dtype)


def far(*shape, dtype=F32):
    return jax.ShapeDtypeStruct(shape, dtype)


def call(kernel, out, *args, scalars=0, held=(), kept=(), scratch=()):
    vmem = pl.BlockSpec(memory_space=pltpu.VMEM)
    smem = pl.BlockSpec(memory_space=pltpu.SMEM)
    hbm = pl.BlockSpec(memory_space=pltpu.HBM)
    kinds = [smem if i < scalars else hbm if i in held else vmem for i in range(len(args))]
    placed = [
        x if kind is smem else pltpu.with_memory_space_constraint(x, kind.memory_space)
        for x, kind in zip(args, kinds)
    ]
    return pl.pallas_call(
        kernel,
        out_shape=out,
        in_specs=kinds,
        out_specs=tuple(hbm if i in kept else vmem for i in range(len(out)))
        if isinstance(out, tuple)
        else vmem,
        scratch_shapes=list(scratch),
        compiler_params=pltpu.CompilerParams(vmem_limit_bytes=24 << 20),
    )(*placed)


def fetched(far, start, held, arrived):
    copies = []
    for j in range(arrived.shape[0]):
        columns = pl.ds(pl.multiple_of(start + j * BLOCK, BLOCK), BLOCK)
        to = held.at[:, pl.ds(j * BLOCK, BLOCK)]
        copies.append(pltpu.make_async_copy(far.at[:, columns], to, arrived.at[j]))
        copies[-1].start()
    return copies


def side_kernel(core, h_far, g_far, out, arrived, came):
    half = g_far.shape[1] // 2
    copies = fetched(g_far, (1 - core[0]) * half, out, arrived)
    copies.append(pltpu.make_async_copy(h_far, out.at[:, half:], came))
    copies[-1].start()
    for copy in copies:
        copy.wait()


def partial_kernel(
    scale, core, turn, x_peer, h_far, w_far, g_far, out, hidden, weight, g_own, arrived, came
):
    half = g_own.shape[1]
    first = [
        pltpu.make_async_copy(h_far, hidden, came.at[0]),
        pltpu.make_async_copy(w_far, weight, came.at[1]),
    ]
    for copy in first:
        copy.start()
    copies = fetched(g_far, core[0] * half, g_own, arrived)
    h_peer = x_peer[:, half:].astype(F32).T.astype(BF16)
    for copy in first:
        copy.wait()
    start = turn[0] * PIECE
    sides = [
        weight[:, pl.ds(pl.multiple_of(side * half + start, PIECE), PIECE)].astype(F32)
        for side in range(2)
    ]
    piece = jnp.concatenate(sides + sides, axis=0).astype(BF16)
    for at in range(0, out.shape[0], piece.shape[0]):
        out[at : at + piece.shape[0], half + TAIL :] = piece
    h_own = hidden[...].astype(F32).T.astype(BF16)
    tops = []
    for copy, at in zip(copies, blocks_of(half)):
        total = dot(h_peer, x_peer[:, at], (1, 0))
        copy.wait()
        total = total + dot(h_own, g_own[:, at], (1, 0))
        out[:, at], top = code(total * scale)
        tops.append(top)
    out[:, half : half + TAIL] = tail_of(tops)


def start_kernel(core, q_t, out):
    half = out.shape[1]
    start = pl.multiple_of(core[0] * half, half)
    out[...] = nn(inverse_factor(nt(q_t[...], q_t[...])), q_t[:, pl.ds(start, half)])


def tail_at(terms, half):
    return terms[:, half : half + TAIL].astype(F32)


def merge_kernel(core, terms, e_own, e_peer, own, peer, piece, copies):
    rows, half = e_own.shape
    n_rep = copies.shape[0]
    left = core[0] == 0
    tops = []
    for j, at in enumerate(blocks_of(half)):
        mine, other = e_own[:, at], e_peer[:, at]
        total = jnp.concatenate(
            [jnp.where(left, mine, other), jnp.where(left, other, mine)], axis=0
        )
        for source in range(terms.shape[0]):
            tail = tail_at(terms[source], half)
            total = total + decode(terms[source, :, at], tail[:, LANES * j : LANES * j + 1])
        own[:, at] = jnp.where(left, total[:rows], total[rows:])
        peer[:, at] = jnp.where(left, total[rows:], total[:rows])
        coded, top = code(total)
        tops.append(top)
        for target in range(n_rep):
            copies[target, :, at] = coded
    tail = tail_of(tops)
    for target in range(n_rep):
        copies[target, :, half:] = tail
    piece[...] = terms[:, :, half + TAIL :]


def sum_kernel(merged, copies):
    half = copies.shape[2] - TAIL
    tops = []
    for j, at in enumerate(blocks_of(half)):
        total = 0.0
        for source in range(merged.shape[0]):
            tail = tail_at(merged[source], half)
            total = total + decode(merged[source, :, at], tail[:, LANES * j : LANES * j + 1])
        coded, top = code(total)
        tops.append(top)
        for target in range(copies.shape[0]):
            copies[target, :, at] = coded
    tail = tail_of(tops)
    for target in range(copies.shape[0]):
        copies[target, :, half:] = tail


def weight_kernel(turn, *refs):
    *pieces, out = refs
    for step, piece in enumerate(pieces):
        place = lax.rem(turn[0] + step, len(pieces))
        out[:, :, pl.ds(pl.multiple_of(place * PIECE, PIECE), PIECE)] = piece[...]


def hidden_kernel(rows, core, w_own, w_peer, g_far, out, g, arrived):
    half = w_own.shape[1]
    copies = fetched(g_far, 0, g, arrived)
    sums = [[0.0, 0.0], [0.0, 0.0]]
    for j, (copy, at) in enumerate(zip(copies, blocks_of(2 * half))):
        copy.wait()
        side = j * BLOCK // half
        columns = pl.ds(j * BLOCK % half, BLOCK)
        for which, weight in enumerate((w_own, w_peer)):
            sums[which][side] = sums[which][side] + dot(g[:, at], weight[:, columns], (1, 1))
    lane = lax.broadcasted_iota(jnp.int32, out.shape, 1)
    first = lane // rows % 2 == 0
    whole = []
    for which in range(2):
        term = jnp.where(first, sums[which][0], sums[which][1])
        width = term.shape[1]
        other = jnp.where(
            first, pltpu.roll(term, width - rows, 1), pltpu.roll(term, rows, 1)
        )
        whole.append(term + other)
    out[...] = jnp.where(first == (core[0] == 0), whole[0], whole[1]).astype(BF16)


def gram_kernel(q_t, coded, high_far, low_far, out, high, low, sent):
    rank, half = q_t.shape
    rows = coded.shape[1]
    for pair in range(coded.shape[0] // 2):
        tails = [coded[2 * pair + k, :, half:].astype(F32) for k in range(2)]
        for j, at in enumerate(blocks_of(half)):
            values = [
                decode(coded[2 * pair + k, :, at], tails[k][:, LANES * j : LANES * j + 1])
                for k in range(2)
            ]
            to = pl.ds(2 * rows * pair, 2 * rows)
            high[to, at], low[to, at] = parts(jnp.concatenate(values, axis=0))
    store = [
        pltpu.make_async_copy(high, high_far, sent.at[0]),
        pltpu.make_async_copy(low, low_far, sent.at[1]),
    ]
    for copy in store:
        copy.start()
    summed = high[...], low[...]
    out[:rank, :] = dot3(parts(q_t[...]), summed, (1, 1))
    cross = dot(summed[0], summed[1], (1, 1))
    out[rank:, :] = dot(summed[0], summed[0], (1, 1)) + (cross + cross.T)
    for copy in store:
        copy.wait()


def power_kernel(own, peer, high_far, low_far, p_out, q_out, high, low, arrived):
    fetch = [
        pltpu.make_async_copy(high_far, high, arrived.at[0]),
        pltpu.make_async_copy(low_far, low, arrived.at[1]),
    ]
    for copy in fetch:
        copy.start()
    rank = p_out.shape[0]
    both = own[...] + peer[...]
    gram = both[rank:]
    p = orth_t(both[:rank])
    y = nn(p, gram)
    p = orth_t(nn(inverse_factor(nt(p, y)), y))
    p_out[...] = p
    for copy in fetch:
        copy.wait()
    q_out[...] = dot3(parts(p), (high[...], low[...]), (1, 0))


def last_kernel(n_rep, core, row, q_own, q_peer, p_t, m_own, m_peer, q_out, update, error):
    rows, half = m_peer.shape
    width = p_t.shape[1]
    want = row[0] + lax.broadcasted_iota(jnp.int32, (8, width), 0)
    pick = jnp.where(lax.broadcasted_iota(jnp.int32, (8, width), 1) == want, 1.0, 0.0)
    p_rows = nt(pick.astype(F32), p_t[...])
    left = core[0] == 0
    for side in range(2):
        at = pl.ds(side * half, half)
        mine = left if side == 0 else jnp.logical_not(left)
        q = jnp.where(mine, q_own[...], q_peer[...])
        merged = jnp.where(mine, m_own[...], m_peer[...])
        q_out[:, at] = q
        step = nn(p_rows, q)[:rows]
        update[:, at] = step
        error[:, at] = merged - step * (1.0 / n_rep)


def swap(x):
    return lax.ppermute(x, CORE, [(0, 1), (1, 0)])


def side_of(x, side):
    half = x.shape[-1] // 2
    return lax.dynamic_slice_in_dim(x, side * half, half, x.ndim - 1)


def exchange(blocks, axes):
    return lax.all_to_all(blocks, axes, 0, 0, tiled=True)


def body(hidden, grad_out, weight_band, error_feedback, q_start):
    n_rep = lax.axis_size(REP)
    chips = lax.axis_size(CHIPS)
    tokens, units = hidden.shape
    scale = 1.0 / math.sqrt(tokens * lax.axis_size(SHARD) * n_rep)
    core = lax.axis_index(CORE)
    core_s = core.astype(jnp.int32)[None]
    row = (lax.axis_index(SHARD) * weight_band.shape[0]).astype(jnp.int32)[None]
    rows = weight_band.shape[0]
    half = grad_out.shape[1] // 2
    rank = q_start.shape[1]

    blocks = pltpu.SemaphoreType.DMA((half // BLOCK,))
    x_send = call(
        side_kernel,
        near(tokens, half + units, dtype=BF16),
        core_s,
        hidden,
        grad_out,
        scalars=1,
        held=(1, 2),
        scratch=(blocks, pltpu.SemaphoreType.DMA(())),
    )
    turn = lax.axis_index("rep_1").astype(jnp.int32)[None]
    terms = call(
        lambda *refs: partial_kernel(scale, *refs),
        far(units, half + TAIL + PIECE, dtype=BF16),
        core_s,
        turn,
        swap(x_send),
        hidden,
        weight_band,
        grad_out,
        scalars=2,
        held=(3, 4, 5),
        scratch=(
            pltpu.VMEM(hidden.shape, BF16),
            pltpu.VMEM(weight_band.shape, BF16),
            pltpu.VMEM((tokens, half), BF16),
            blocks,
            pltpu.SemaphoreType.DMA((2,)),
        ),
    )
    terms = exchange(terms.reshape(chips, 2 * rows, -1), CHIPS)

    e_own = side_of(error_feedback[0], core)
    e_peer = swap(side_of(error_feedback[0], 1 - core))
    q_t = call(start_kernel, near(rank, half), core_s, q_start.T, scalars=1)
    terms, q_t = lax.optimization_barrier((terms, q_t))

    m_own, m_send, piece, copies = call(
        merge_kernel,
        (
            near(rows, half),
            near(rows, half),
            near(chips, 2 * rows, PIECE, dtype=BF16),
            near(n_rep, 2 * rows, half + TAIL, dtype=BF16),
        ),
        core_s,
        terms,
        e_own,
        e_peer,
        scalars=1,
    )
    merged = exchange(copies, REP)
    copies = call(sum_kernel, far(chips, 2 * rows, half + TAIL, dtype=BF16), merged)
    coded = exchange(copies, CHIPS)

    turns = lax.axis_size("rep_1")
    pieces = [piece]
    for step in range(1, turns):
        move = [(i, (i - step) % turns) for i in range(turns)]
        pieces.append(lax.ppermute(piece, "rep_1", move))
    w_own = call(
        weight_kernel, near(chips, 2 * rows, half, dtype=BF16), turn, *pieces, scalars=1
    )
    w_own = w_own.reshape(units, half)
    d_hidden = call(
        lambda *refs: hidden_kernel(rows, *refs),
        far(tokens, units, dtype=BF16),
        core_s,
        w_own,
        swap(w_own),
        grad_out,
        scalars=1,
        held=(3,),
        scratch=(
            pltpu.VMEM((tokens, 2 * half), BF16),
            pltpu.SemaphoreType.DMA((2 * half // BLOCK,)),
        ),
    )
    m_peer = swap(m_send)
    coded, m_peer, d_hidden = lax.optimization_barrier((coded, m_peer, d_hidden))
    halves = (
        pltpu.VMEM((units, half), BF16),
        pltpu.VMEM((units, half), BF16),
        pltpu.SemaphoreType.DMA((2,)),
    )
    high, low, grams = call(
        gram_kernel,
        (
            pltpu.HBM((units, half), BF16),
            pltpu.HBM((units, half), BF16),
            near(rank + units, units),
        ),
        q_t,
        coded,
        kept=(0, 1),
        scratch=halves,
    )
    p_t, q_own = call(
        power_kernel,
        (near(rank, units), near(rank, half)),
        grams,
        swap(grams),
        high,
        low,
        held=(2, 3),
        scratch=halves,
    )
    q_next, update, error = call(
        lambda *refs: last_kernel(n_rep, *refs),
        (far(rank, 2 * half), far(rows, 2 * half), far(rows, 2 * half)),
        core_s,
        row,
        q_own,
        swap(q_own),
        p_t,
        m_own,
        m_peer,
        scalars=2,
    )
    return (update, error[None], q_next.T, d_hidden)


def solution(mesh):
    finer = Mesh(
        mesh.devices.reshape(2, mesh.shape["rep"] // 2, 4, 8, 2), REP_SHARD
    )
    placed = (P(REP_SHARD, None), P(REP_SHARD, None), P(SHARD, None), P(REP, SHARD, None), P())
    return jax.shard_map(
        body,
        mesh=finer,
        in_specs=placed,
        out_specs=(P(SHARD, None), P(REP, SHARD, None), P(), P(REP_SHARD, None)),
        check_vma=False,
    )
```

```python
import math

import jax
import jax.numpy as jnp
from jax import lax
from jax.experimental import pallas as pl
from jax.experimental.pallas import tpu as pltpu
from jax.sharding import Mesh
from jax.sharding import PartitionSpec as P

SHARD = ("shard_0", "shard_1", "shard_2")
REP = ("rep_0", "rep_1")
REP_SHARD = REP + SHARD
CHIPS = ("shard_0", "shard_1")
CORE = "shard_2"
HIGHEST = lax.Precision.HIGHEST
F32, BF16 = jnp.float32, jnp.bfloat16
SPAN = 250.0
LN2 = math.log(2.0)
BLOCK = 512
TAIL = 128
LANES = 32
PANEL = 8
PIECE = 512


def dot(a, b, over, precision=None):
    return lax.dot_general(
        a, b, ((over[:1], over[1:]), ((), ())), precision=precision, preferred_element_type=F32
    )


def nn(a, b):
    return dot(a, b, (1, 0), HIGHEST)


def nt(a, b):
    return dot(a, b, (1, 1), HIGHEST)


def parts(x):
    high = x.astype(BF16)
    return high, (x - high.astype(F32)).astype(BF16)


def dot3(a, b, over):
    return dot(a[0], b[0], over) + (dot(a[0], b[1], over) + dot(a[1], b[0], over))


def inverse_factor(gram):
    n = gram.shape[0]
    rows = lax.broadcasted_iota(jnp.int32, (n, n), 0)
    cols = lax.broadcasted_iota(jnp.int32, (n, n), 1)
    a, b = gram, jnp.where(rows == cols, 1.0, 0.0).astype(F32)
    for j in range(0, n, PANEL):
        tall = [jnp.broadcast_to(a[:, j + m : j + m + 1], (n, n)) for m in range(PANEL)]
        left = [a[j + m : j + m + 1, :] for m in range(PANEL)]
        right = [b[j + m : j + m + 1, :] for m in range(PANEL)]
        for m in range(PANEL):
            at = j + m
            tall[m] = jnp.where(rows > at, tall[m] * (1.0 / tall[m][at : at + 1, :]), 0.0)
            for k in range(m + 1, PANEL):
                tall[k] = tall[k] - tall[m] * tall[k][at : at + 1, :]
                factor = tall[m][j + k : j + k + 1, :]
                left[k], right[k] = left[k] - factor * left[m], right[k] - factor * right[m]
        for m in range(PANEL):
            a, b = a - tall[m] * left[m], b - tall[m] * right[m]
    pivots = jnp.sum(jnp.where(rows == cols, a, 0.0), axis=1, keepdims=True)
    return b * (1.0 / jnp.sqrt(pivots))


def orth_t(x):
    return nn(inverse_factor(nt(x, x)), x)


def code(x):
    top = jnp.max(jnp.abs(x), axis=1, keepdims=True)
    top = jnp.maximum(top * 1.01, 1e-30).astype(BF16).astype(F32)
    level = jnp.sqrt(jnp.abs(x) * (1.0 / top))
    size = jnp.exp(level * (SPAN * LN2) - (SPAN * LN2 / 2))
    return jnp.where(x < 0, -size, size).astype(BF16), top


def decode(y, top):
    y = y.astype(F32)
    level = jnp.log(jnp.abs(y)) * (1.0 / (SPAN * LN2)) + 0.5
    size = level * level * top
    return jnp.where(y < 0, -size, size)


def tail_of(tops):
    wide = [jnp.broadcast_to(top, (top.shape[0], LANES)) for top in tops]
    return jnp.concatenate(wide, axis=1).astype(BF16)


def blocks_of(half):
    return [pl.ds(j * BLOCK, BLOCK) for j in range(half // BLOCK)]


def near(*shape, dtype=F32):
    return pltpu.VMEM(shape, dtype)


def far(*shape, dtype=F32):
    return jax.ShapeDtypeStruct(shape, dtype)


def call(kernel, out, *args, scalars=0, held=(), kept=(), scratch=()):
    vmem = pl.BlockSpec(memory_space=pltpu.VMEM)
    smem = pl.BlockSpec(memory_space=pltpu.SMEM)
    hbm = pl.BlockSpec(memory_space=pltpu.HBM)
    kinds = [smem if i < scalars else hbm if i in held else vmem for i in range(len(args))]
    placed = [
        x if kind is smem else pltpu.with_memory_space_constraint(x, kind.memory_space)
        for x, kind in zip(args, kinds)
    ]
    return pl.pallas_call(
        kernel,
        out_shape=out,
        in_specs=kinds,
        out_specs=tuple(hbm if i in kept else vmem for i in range(len(out)))
        if isinstance(out, tuple)
        else vmem,
        scratch_shapes=list(scratch),
        compiler_params=pltpu.CompilerParams(vmem_limit_bytes=24 << 20),
    )(*placed)


def fetched(far, start, held, arrived):
    copies = []
    for j in range(arrived.shape[0]):
        columns = pl.ds(pl.multiple_of(start + j * BLOCK, BLOCK), BLOCK)
        to = held.at[:, pl.ds(j * BLOCK, BLOCK)]
        copies.append(pltpu.make_async_copy(far.at[:, columns], to, arrived.at[j]))
        copies[-1].start()
    return copies


def side_kernel(core, h_far, g_far, out, arrived, came):
    half = g_far.shape[1] // 2
    copies = fetched(g_far, (1 - core[0]) * half, out, arrived)
    copies.append(pltpu.make_async_copy(h_far, out.at[:, half:], came))
    copies[-1].start()
    for copy in copies:
        copy.wait()


def partial_kernel(
    scale, core, turn, x_peer, h_far, w_far, g_far, out, hidden, weight, g_own, arrived, came
):
    half = g_own.shape[1]
    first = [
        pltpu.make_async_copy(h_far, hidden, came.at[0]),
        pltpu.make_async_copy(w_far, weight, came.at[1]),
    ]
    for copy in first:
        copy.start()
    copies = fetched(g_far, core[0] * half, g_own, arrived)
    h_peer = x_peer[:, half:].astype(F32).T.astype(BF16)
    for copy in first:
        copy.wait()
    start = turn[0] * PIECE
    sides = [
        weight[:, pl.ds(pl.multiple_of(side * half + start, PIECE), PIECE)].astype(F32)
        for side in range(2)
    ]
    piece = jnp.concatenate(sides + sides, axis=0).astype(BF16)
    for at in range(0, out.shape[0], piece.shape[0]):
        out[at : at + piece.shape[0], half + TAIL :] = piece
    h_own = hidden[...].astype(F32).T.astype(BF16)
    tops = []
    for copy, at in zip(copies, blocks_of(half)):
        total = dot(h_peer, x_peer[:, at], (1, 0))
        copy.wait()
        total = total + dot(h_own, g_own[:, at], (1, 0))
        out[:, at], top = code(total * scale)
        tops.append(top)
    out[:, half : half + TAIL] = tail_of(tops)


def start_kernel(core, q_t, own, peer):
    half = own.shape[1]
    inverse = inverse_factor(nt(q_t[...], q_t[...]))
    for out, side in ((own, core[0]), (peer, 1 - core[0])):
        out[...] = nn(inverse, q_t[:, pl.ds(pl.multiple_of(side * half, half), half)])


def tail_at(terms, half):
    return terms[:, half : half + TAIL].astype(F32)


def merge_kernel(core, terms, e_own, e_peer, own, peer, piece, copies):
    rows, half = e_own.shape
    n_rep = copies.shape[0]
    left = core[0] == 0
    tops = []
    for j, at in enumerate(blocks_of(half)):
        mine, other = e_own[:, at], e_peer[:, at]
        total = jnp.concatenate(
            [jnp.where(left, mine, other), jnp.where(left, other, mine)], axis=0
        )
        for source in range(terms.shape[0]):
            tail = tail_at(terms[source], half)
            total = total + decode(terms[source, :, at], tail[:, LANES * j : LANES * j + 1])
        own[:, at] = jnp.where(left, total[:rows], total[rows:])
        peer[:, at] = jnp.where(left, total[rows:], total[:rows])
        coded, top = code(total)
        tops.append(top)
        for target in range(n_rep):
            copies[target, :, at] = coded
    tail = tail_of(tops)
    for target in range(n_rep):
        copies[target, :, half:] = tail
    piece[...] = terms[:, :, half + TAIL :]


def sum_kernel(merged, copies):
    half = copies.shape[2] - TAIL
    tops = []
    for j, at in enumerate(blocks_of(half)):
        total = 0.0
        for source in range(merged.shape[0]):
            tail = tail_at(merged[source], half)
            total = total + decode(merged[source, :, at], tail[:, LANES * j : LANES * j + 1])
        coded, top = code(total)
        tops.append(top)
        for target in range(copies.shape[0]):
            copies[target, :, at] = coded
    tail = tail_of(tops)
    for target in range(copies.shape[0]):
        copies[target, :, half:] = tail


def weight_kernel(turn, *refs):
    *pieces, out = refs
    for step, piece in enumerate(pieces):
        place = lax.rem(turn[0] + step, len(pieces))
        out[:, :, pl.ds(pl.multiple_of(place * PIECE, PIECE), PIECE)] = piece[...]


def hidden_kernel(rows, core, w_own, w_peer, g_far, out, g, arrived):
    half = w_own.shape[1]
    copies = fetched(g_far, 0, g, arrived)
    sums = [[0.0, 0.0], [0.0, 0.0]]
    for j, (copy, at) in enumerate(zip(copies, blocks_of(2 * half))):
        copy.wait()
        side = j * BLOCK // half
        columns = pl.ds(j * BLOCK % half, BLOCK)
        for which, weight in enumerate((w_own, w_peer)):
            sums[which][side] = sums[which][side] + dot(g[:, at], weight[:, columns], (1, 1))
    lane = lax.broadcasted_iota(jnp.int32, out.shape, 1)
    first = lane // rows % 2 == 0
    whole = []
    for which in range(2):
        term = jnp.where(first, sums[which][0], sums[which][1])
        width = term.shape[1]
        other = jnp.where(
            first, pltpu.roll(term, width - rows, 1), pltpu.roll(term, rows, 1)
        )
        whole.append(term + other)
    out[...] = jnp.where(first == (core[0] == 0), whole[0], whole[1]).astype(BF16)


def unpack(coded, high, low):
    rows, half = coded.shape[1], high.shape[1]
    for pair in range(coded.shape[0] // 2):
        tails = [tail_at(coded[2 * pair + k], half) for k in range(2)]
        for j, at in enumerate(blocks_of(half)):
            values = [
                decode(coded[2 * pair + k, :, at], tails[k][:, LANES * j : LANES * j + 1])
                for k in range(2)
            ]
            to = pl.ds(2 * rows * pair, 2 * rows)
            high[to, at], low[to, at] = parts(jnp.concatenate(values, axis=0))


def grams_of(q_t, high, low):
    summed = high[...], low[...]
    cross = dot(summed[0], summed[1], (1, 1))
    gram = dot(summed[0], summed[0], (1, 1)) + (cross + cross.T)
    return dot3(parts(q_t[...]), summed, (1, 1)), gram


def gram_kernel(q_t, coded, high_far, low_far, out, high, low, sent):
    rank = q_t.shape[0]
    unpack(coded, high, low)
    store = [
        pltpu.make_async_copy(high, high_far, sent.at[0]),
        pltpu.make_async_copy(low, low_far, sent.at[1]),
    ]
    for copy in store:
        copy.start()
    out[:rank, :], out[rank:, :] = grams_of(q_t, high, low)
    for copy in store:
        copy.wait()


def last_kernel(n_rep, core, row, grams, q_t, coded, m_own, m_peer, high_far, low_far, *refs):
    q_out, update, error, high, low, high_peer, low_peer, arrived = refs
    fetch = [
        pltpu.make_async_copy(high_far, high, arrived.at[0]),
        pltpu.make_async_copy(low_far, low, arrived.at[1]),
    ]
    for copy in fetch:
        copy.start()
    unpack(coded, high_peer, low_peer)
    y, gram = grams_of(q_t, high_peer, low_peer)
    rank = y.shape[0]
    y, gram = grams[:rank, :] + y, grams[rank:, :] + gram
    p = orth_t(y)
    y = nn(p, gram)
    p = orth_t(nn(inverse_factor(nt(p, y)), y))
    for copy in fetch:
        copy.wait()
    q_own = dot3(parts(p), (high[...], low[...]), (1, 0))
    q_peer = dot3(parts(p), (high_peer[...], low_peer[...]), (1, 0))

    rows, half = m_peer.shape
    width = p.shape[1]
    want = row[0] + lax.broadcasted_iota(jnp.int32, (8, width), 0)
    pick = jnp.where(lax.broadcasted_iota(jnp.int32, (8, width), 1) == want, 1.0, 0.0)
    p_rows = nt(pick.astype(F32), p)
    for q, merged, side in ((q_own, m_own, core[0]), (q_peer, m_peer, 1 - core[0])):
        at = pl.ds(pl.multiple_of(side * half, half), half)
        q_out[:, at] = q
        step = nn(p_rows, q)[:rows]
        update[:, at] = step
        error[:, at] = merged[...] - step * (1.0 / n_rep)


def swap(x):
    return lax.ppermute(x, CORE, [(0, 1), (1, 0)])


def side_of(x, side):
    half = x.shape[-1] // 2
    return lax.dynamic_slice_in_dim(x, side * half, half, x.ndim - 1)


def exchange(blocks, axes):
    return lax.all_to_all(blocks, axes, 0, 0, tiled=True)


def body(hidden, grad_out, weight_band, error_feedback, q_start):
    n_rep = lax.axis_size(REP)
    chips = lax.axis_size(CHIPS)
    tokens, units = hidden.shape
    scale = 1.0 / math.sqrt(tokens * lax.axis_size(SHARD) * n_rep)
    core = lax.axis_index(CORE)
    core_s = core.astype(jnp.int32)[None]
    row = (lax.axis_index(SHARD) * weight_band.shape[0]).astype(jnp.int32)[None]
    rows = weight_band.shape[0]
    half = grad_out.shape[1] // 2
    rank = q_start.shape[1]

    blocks = pltpu.SemaphoreType.DMA((half // BLOCK,))
    x_send = call(
        side_kernel,
        near(tokens, half + units, dtype=BF16),
        core_s,
        hidden,
        grad_out,
        scalars=1,
        held=(1, 2),
        scratch=(blocks, pltpu.SemaphoreType.DMA(())),
    )
    turn = lax.axis_index("rep_1").astype(jnp.int32)[None]
    terms = call(
        lambda *refs: partial_kernel(scale, *refs),
        far(units, half + TAIL + PIECE, dtype=BF16),
        core_s,
        turn,
        swap(x_send),
        hidden,
        weight_band,
        grad_out,
        scalars=2,
        held=(3, 4, 5),
        scratch=(
            pltpu.VMEM(hidden.shape, BF16),
            pltpu.VMEM(weight_band.shape, BF16),
            pltpu.VMEM((tokens, half), BF16),
            blocks,
            pltpu.SemaphoreType.DMA((2,)),
        ),
    )
    terms = exchange(terms.reshape(chips, 2 * rows, -1), CHIPS)

    e_own = side_of(error_feedback[0], core)
    e_peer = swap(side_of(error_feedback[0], 1 - core))
    q_t, q_far = call(
        start_kernel, (near(rank, half), near(rank, half)), core_s, q_start.T, scalars=1
    )
    terms, q_t, q_far = lax.optimization_barrier((terms, q_t, q_far))

    m_own, m_send, piece, copies = call(
        merge_kernel,
        (
            near(rows, half),
            near(rows, half),
            near(chips, 2 * rows, PIECE, dtype=BF16),
            near(n_rep, 2 * rows, half + TAIL, dtype=BF16),
        ),
        core_s,
        terms,
        e_own,
        e_peer,
        scalars=1,
    )
    merged = exchange(copies, REP)
    copies = call(sum_kernel, far(chips, 2 * rows, half + TAIL, dtype=BF16), merged)
    coded = exchange(copies, CHIPS)

    turns = lax.axis_size("rep_1")
    pieces = [piece]
    for step in range(1, turns):
        move = [(i, (i - step) % turns) for i in range(turns)]
        pieces.append(lax.ppermute(piece, "rep_1", move))
    w_own = call(
        weight_kernel, near(chips, 2 * rows, half, dtype=BF16), turn, *pieces, scalars=1
    )
    w_own = w_own.reshape(units, half)
    d_hidden = call(
        lambda *refs: hidden_kernel(rows, *refs),
        far(tokens, units, dtype=BF16),
        core_s,
        w_own,
        swap(w_own),
        grad_out,
        scalars=1,
        held=(3,),
        scratch=(
            pltpu.VMEM((tokens, 2 * half), BF16),
            pltpu.SemaphoreType.DMA((2 * half // BLOCK,)),
        ),
    )
    m_peer = swap(m_send)
    coded, m_peer, d_hidden = lax.optimization_barrier((coded, m_peer, d_hidden))
    halves = (
        pltpu.VMEM((units, half), BF16),
        pltpu.VMEM((units, half), BF16),
        pltpu.SemaphoreType.DMA((2,)),
    )
    high, low, grams = call(
        gram_kernel,
        (
            pltpu.HBM((units, half), BF16),
            pltpu.HBM((units, half), BF16),
            near(rank + units, units),
        ),
        q_t,
        coded,
        kept=(0, 1),
        scratch=halves,
    )
    q_next, update, error = call(
        lambda *refs: last_kernel(n_rep, *refs),
        (far(rank, 2 * half), far(rows, 2 * half), far(rows, 2 * half)),
        core_s,
        row,
        grams,
        q_far,
        swap(coded),
        m_own,
        m_peer,
        high,
        low,
        scalars=2,
        held=(7, 8),
        scratch=halves[:2] * 2 + halves[2:],
    )
    return (update, error[None], q_next.T, d_hidden)


def solution(mesh):
    finer = Mesh(
        mesh.devices.reshape(2, mesh.shape["rep"] // 2, 4, 8, 2), REP_SHARD
    )
    placed = (P(REP_SHARD, None), P(REP_SHARD, None), P(SHARD, None), P(REP, SHARD, None), P())
    return jax.shard_map(
        body,
        mesh=finer,
        in_specs=placed,
        out_specs=(P(SHARD, None), P(REP, SHARD, None), P(), P(REP_SHARD, None)),
        check_vma=False,
    )
```

```python
import math

import jax
import jax.numpy as jnp
from jax import lax
from jax.experimental import pallas as pl
from jax.experimental.pallas import tpu as pltpu
from jax.sharding import Mesh
from jax.sharding import PartitionSpec as P

SHARD = ("shard_0", "shard_1", "shard_2")
REP = ("rep_0", "rep_1")
REP_SHARD = REP + SHARD
CHIPS = ("shard_0", "shard_1")
CORE = "shard_2"
HIGHEST = lax.Precision.HIGHEST
F32, BF16 = jnp.float32, jnp.bfloat16
SPAN = 250.0
LN2 = math.log(2.0)
BLOCK = 512
TAIL = 128
LANES = 32
PANEL = 8
PIECE = 512


def dot(a, b, over, precision=None):
    return lax.dot_general(
        a, b, ((over[:1], over[1:]), ((), ())), precision=precision, preferred_element_type=F32
    )


def nn(a, b):
    return dot(a, b, (1, 0), HIGHEST)


def nt(a, b):
    return dot(a, b, (1, 1), HIGHEST)


def parts(x):
    high = x.astype(BF16)
    return high, (x - high.astype(F32)).astype(BF16)


def dot3(a, b, over):
    return dot(a[0], b[0], over) + (dot(a[0], b[1], over) + dot(a[1], b[0], over))


def inverse_factor(gram):
    n = gram.shape[0]
    rows = lax.broadcasted_iota(jnp.int32, (n, n), 0)
    cols = lax.broadcasted_iota(jnp.int32, (n, n), 1)
    a, b = gram, jnp.where(rows == cols, 1.0, 0.0).astype(F32)
    for j in range(0, n, PANEL):
        tall = [jnp.broadcast_to(a[:, j + m : j + m + 1], (n, n)) for m in range(PANEL)]
        left = [a[j + m : j + m + 1, :] for m in range(PANEL)]
        right = [b[j + m : j + m + 1, :] for m in range(PANEL)]
        for m in range(PANEL):
            at = j + m
            tall[m] = jnp.where(rows > at, tall[m] * (1.0 / tall[m][at : at + 1, :]), 0.0)
            for k in range(m + 1, PANEL):
                tall[k] = tall[k] - tall[m] * tall[k][at : at + 1, :]
                factor = tall[m][j + k : j + k + 1, :]
                left[k], right[k] = left[k] - factor * left[m], right[k] - factor * right[m]
        for m in range(PANEL):
            a, b = a - tall[m] * left[m], b - tall[m] * right[m]
    pivots = jnp.sum(jnp.where(rows == cols, a, 0.0), axis=1, keepdims=True)
    return b * (1.0 / jnp.sqrt(pivots))


def orth_t(x):
    return nn(inverse_factor(nt(x, x)), x)


def code(x):
    top = jnp.max(jnp.abs(x), axis=1, keepdims=True)
    top = jnp.maximum(top * 1.01, 1e-30).astype(BF16).astype(F32)
    level = jnp.sqrt(jnp.abs(x) * (1.0 / top))
    size = jnp.exp(level * (SPAN * LN2) - (SPAN * LN2 / 2))
    return jnp.where(x < 0, -size, size).astype(BF16), top


def decode(y, top):
    y = y.astype(F32)
    level = jnp.log(jnp.abs(y)) * (1.0 / (SPAN * LN2)) + 0.5
    size = level * level * top
    return jnp.where(y < 0, -size, size)


def tail_of(tops):
    wide = [jnp.broadcast_to(top, (top.shape[0], LANES)) for top in tops]
    return jnp.concatenate(wide, axis=1).astype(BF16)


def blocks_of(half):
    return [pl.ds(j * BLOCK, BLOCK) for j in range(half // BLOCK)]


def near(*shape, dtype=F32):
    return pltpu.VMEM(shape, dtype)


def far(*shape, dtype=F32):
    return jax.ShapeDtypeStruct(shape, dtype)


def call(kernel, out, *args, scalars=0, held=(), kept=(), scratch=()):
    vmem = pl.BlockSpec(memory_space=pltpu.VMEM)
    smem = pl.BlockSpec(memory_space=pltpu.SMEM)
    hbm = pl.BlockSpec(memory_space=pltpu.HBM)
    kinds = [smem if i < scalars else hbm if i in held else vmem for i in range(len(args))]
    placed = [
        x if kind is smem else pltpu.with_memory_space_constraint(x, kind.memory_space)
        for x, kind in zip(args, kinds)
    ]
    return pl.pallas_call(
        kernel,
        out_shape=out,
        in_specs=kinds,
        out_specs=tuple(hbm if i in kept else vmem for i in range(len(out)))
        if isinstance(out, tuple)
        else vmem,
        scratch_shapes=list(scratch),
        compiler_params=pltpu.CompilerParams(vmem_limit_bytes=24 << 20),
    )(*placed)


def fetched(far, start, held, arrived):
    copies = []
    for j in range(arrived.shape[0]):
        columns = pl.ds(pl.multiple_of(start + j * BLOCK, BLOCK), BLOCK)
        to = held.at[:, pl.ds(j * BLOCK, BLOCK)]
        copies.append(pltpu.make_async_copy(far.at[:, columns], to, arrived.at[j]))
        copies[-1].start()
    return copies


def side_kernel(core, h_far, g_far, out, arrived, came):
    half = g_far.shape[1] // 2
    copies = fetched(g_far, (1 - core[0]) * half, out, arrived)
    copies.append(pltpu.make_async_copy(h_far, out.at[:, half:], came))
    copies[-1].start()
    for copy in copies:
        copy.wait()


def partial_kernel(
    scale, core, turn, x_peer, h_far, w_far, g_far, out, hidden, weight, g_own, arrived, came
):
    half = g_own.shape[1]
    first = [
        pltpu.make_async_copy(h_far, hidden, came.at[0]),
        pltpu.make_async_copy(w_far, weight, came.at[1]),
    ]
    for copy in first:
        copy.start()
    copies = fetched(g_far, core[0] * half, g_own, arrived)
    h_peer = x_peer[:, half:].astype(F32).T.astype(BF16)
    for copy in first:
        copy.wait()
    start = turn[0] * PIECE
    sides = [
        weight[:, pl.ds(pl.multiple_of(side * half + start, PIECE), PIECE)].astype(F32)
        for side in range(2)
    ]
    piece = jnp.concatenate(sides + sides, axis=0).astype(BF16)
    for at in range(0, out.shape[0], piece.shape[0]):
        out[at : at + piece.shape[0], half + TAIL :] = piece
    h_own = hidden[...].astype(F32).T.astype(BF16)
    tops = []
    for copy, at in zip(copies, blocks_of(half)):
        total = dot(h_peer, x_peer[:, at], (1, 0))
        copy.wait()
        total = total + dot(h_own, g_own[:, at], (1, 0))
        out[:, at], top = code(total * scale)
        tops.append(top)
    out[:, half : half + TAIL] = tail_of(tops)


def start_kernel(core, q_t, own, peer):
    half = own.shape[1]
    inverse = inverse_factor(nt(q_t[...], q_t[...]))
    for out, side in ((own, core[0]), (peer, 1 - core[0])):
        out[...] = nn(inverse, q_t[:, pl.ds(pl.multiple_of(side * half, half), half)])


def tail_at(terms, half):
    return terms[:, half : half + TAIL].astype(F32)


def merge_kernel(core, terms, e_own, e_peer, own, peer, piece, copies):
    rows, half = e_own.shape
    n_rep = copies.shape[0]
    left = core[0] == 0
    tops = []
    for j, at in enumerate(blocks_of(half)):
        mine, other = e_own[:, at], e_peer[:, at]
        total = jnp.concatenate(
            [jnp.where(left, mine, other), jnp.where(left, other, mine)], axis=0
        )
        for source in range(terms.shape[0]):
            tail = tail_at(terms[source], half)
            total = total + decode(terms[source, :, at], tail[:, LANES * j : LANES * j + 1])
        own[:, at] = jnp.where(left, total[:rows], total[rows:])
        peer[:, at] = jnp.where(left, total[rows:], total[:rows])
        coded, top = code(total)
        tops.append(top)
        for target in range(n_rep):
            copies[target, :, at] = coded
    tail = tail_of(tops)
    for target in range(n_rep):
        copies[target, :, half:] = tail
    piece[...] = terms[:, :, half + TAIL :]


def sum_kernel(merged, copies):
    half = copies.shape[2] - TAIL
    tops = []
    for j, at in enumerate(blocks_of(half)):
        total = 0.0
        for source in range(merged.shape[0]):
            tail = tail_at(merged[source], half)
            total = total + decode(merged[source, :, at], tail[:, LANES * j : LANES * j + 1])
        coded, top = code(total)
        tops.append(top)
        for target in range(copies.shape[0]):
            copies[target, :, at] = coded
    tail = tail_of(tops)
    for target in range(copies.shape[0]):
        copies[target, :, half:] = tail


def weight_kernel(turn, *refs):
    *pieces, merged, out = refs
    chips = pieces[0].shape[0]
    for step, piece in enumerate(pieces):
        place = lax.rem(turn[0] + step, len(pieces))
        out[:chips, :, pl.ds(pl.multiple_of(place * PIECE, PIECE), PIECE)] = piece[...]
    high, low = parts(merged[...])
    both = jnp.concatenate([high.astype(F32), low.astype(F32)], axis=0)
    out[chips] = both.astype(BF16)


def hidden_kernel(rows, core, w_own, w_peer, g_far, out, merged, g, arrived):
    half = w_own.shape[1]
    units = out.shape[1]
    copies = fetched(g_far, 0, g, arrived)
    both = w_peer[units:, :].astype(F32)
    merged[...] = both[:rows] + both[rows:]
    sums = [[0.0, 0.0], [0.0, 0.0]]
    for j, (copy, at) in enumerate(zip(copies, blocks_of(2 * half))):
        copy.wait()
        side = j * BLOCK // half
        columns = pl.ds(j * BLOCK % half, BLOCK)
        for which, weight in enumerate((w_own, w_peer)):
            sums[which][side] = sums[which][side] + dot(
                g[:, at], weight[:units, columns], (1, 1)
            )
    lane = lax.broadcasted_iota(jnp.int32, out.shape, 1)
    first = lane // rows % 2 == 0
    whole = []
    for which in range(2):
        term = jnp.where(first, sums[which][0], sums[which][1])
        width = term.shape[1]
        other = jnp.where(
            first, pltpu.roll(term, width - rows, 1), pltpu.roll(term, rows, 1)
        )
        whole.append(term + other)
    out[...] = jnp.where(first == (core[0] == 0), whole[0], whole[1]).astype(BF16)


def unpack(coded, high, low):
    rows, half = coded.shape[1], high.shape[1]
    for pair in range(coded.shape[0] // 2):
        tails = [tail_at(coded[2 * pair + k], half) for k in range(2)]
        for j, at in enumerate(blocks_of(half)):
            values = [
                decode(coded[2 * pair + k, :, at], tails[k][:, LANES * j : LANES * j + 1])
                for k in range(2)
            ]
            to = pl.ds(2 * rows * pair, 2 * rows)
            high[to, at], low[to, at] = parts(jnp.concatenate(values, axis=0))


def grams_of(q_t, high, low):
    summed = high[...], low[...]
    cross = dot(summed[0], summed[1], (1, 1))
    gram = dot(summed[0], summed[0], (1, 1)) + (cross + cross.T)
    return dot3(parts(q_t[...]), summed, (1, 1)), gram


def gram_kernel(q_t, coded, high_far, low_far, out, high, low, sent):
    rank = q_t.shape[0]
    unpack(coded, high, low)
    store = [
        pltpu.make_async_copy(high, high_far, sent.at[0]),
        pltpu.make_async_copy(low, low_far, sent.at[1]),
    ]
    for copy in store:
        copy.start()
    out[:rank, :], out[rank:, :] = grams_of(q_t, high, low)
    for copy in store:
        copy.wait()


def last_kernel(n_rep, core, row, grams, q_t, coded, m_own, m_peer, high_far, low_far, *refs):
    q_out, update, error, high, low, high_peer, low_peer, arrived = refs
    fetch = [
        pltpu.make_async_copy(high_far, high, arrived.at[0]),
        pltpu.make_async_copy(low_far, low, arrived.at[1]),
    ]
    for copy in fetch:
        copy.start()
    unpack(coded, high_peer, low_peer)
    y, gram = grams_of(q_t, high_peer, low_peer)
    rank = y.shape[0]
    y, gram = grams[:rank, :] + y, grams[rank:, :] + gram
    p = orth_t(y)
    y = nn(p, gram)
    p = orth_t(nn(inverse_factor(nt(p, y)), y))
    for copy in fetch:
        copy.wait()
    q_own = dot3(parts(p), (high[...], low[...]), (1, 0))
    q_peer = dot3(parts(p), (high_peer[...], low_peer[...]), (1, 0))

    rows, half = m_peer.shape
    width = p.shape[1]
    want = row[0] + lax.broadcasted_iota(jnp.int32, (8, width), 0)
    pick = jnp.where(lax.broadcasted_iota(jnp.int32, (8, width), 1) == want, 1.0, 0.0)
    p_rows = nt(pick.astype(F32), p)
    for q, merged, side in ((q_own, m_own, core[0]), (q_peer, m_peer, 1 - core[0])):
        at = pl.ds(pl.multiple_of(side * half, half), half)
        q_out[:, at] = q
        step = nn(p_rows, q)[:rows]
        update[:, at] = step
        error[:, at] = merged[...] - step * (1.0 / n_rep)


def swap(x):
    return lax.ppermute(x, CORE, [(0, 1), (1, 0)])


def side_of(x, side):
    half = x.shape[-1] // 2
    return lax.dynamic_slice_in_dim(x, side * half, half, x.ndim - 1)


def exchange(blocks, axes):
    return lax.all_to_all(blocks, axes, 0, 0, tiled=True)


def body(hidden, grad_out, weight_band, error_feedback, q_start):
    n_rep = lax.axis_size(REP)
    chips = lax.axis_size(CHIPS)
    tokens, units = hidden.shape
    scale = 1.0 / math.sqrt(tokens * lax.axis_size(SHARD) * n_rep)
    core = lax.axis_index(CORE)
    core_s = core.astype(jnp.int32)[None]
    row = (lax.axis_index(SHARD) * weight_band.shape[0]).astype(jnp.int32)[None]
    rows = weight_band.shape[0]
    half = grad_out.shape[1] // 2
    rank = q_start.shape[1]

    blocks = pltpu.SemaphoreType.DMA((half // BLOCK,))
    x_send = call(
        side_kernel,
        near(tokens, half + units, dtype=BF16),
        core_s,
        hidden,
        grad_out,
        scalars=1,
        held=(1, 2),
        scratch=(blocks, pltpu.SemaphoreType.DMA(())),
    )
    turn = lax.axis_index("rep_1").astype(jnp.int32)[None]
    terms = call(
        lambda *refs: partial_kernel(scale, *refs),
        far(units, half + TAIL + PIECE, dtype=BF16),
        core_s,
        turn,
        swap(x_send),
        hidden,
        weight_band,
        grad_out,
        scalars=2,
        held=(3, 4, 5),
        scratch=(
            pltpu.VMEM(hidden.shape, BF16),
            pltpu.VMEM(weight_band.shape, BF16),
            pltpu.VMEM((tokens, half), BF16),
            blocks,
            pltpu.SemaphoreType.DMA((2,)),
        ),
    )
    terms = exchange(terms.reshape(chips, 2 * rows, -1), CHIPS)

    e_own = side_of(error_feedback[0], core)
    e_peer = swap(side_of(error_feedback[0], 1 - core))
    q_t, q_far = call(
        start_kernel, (near(rank, half), near(rank, half)), core_s, q_start.T, scalars=1
    )
    terms, q_t, q_far = lax.optimization_barrier((terms, q_t, q_far))

    m_own, m_send, piece, copies = call(
        merge_kernel,
        (
            near(rows, half),
            near(rows, half),
            near(chips, 2 * rows, PIECE, dtype=BF16),
            near(n_rep, 2 * rows, half + TAIL, dtype=BF16),
        ),
        core_s,
        terms,
        e_own,
        e_peer,
        scalars=1,
    )
    merged = exchange(copies, REP)
    copies = call(sum_kernel, far(chips, 2 * rows, half + TAIL, dtype=BF16), merged)
    coded = exchange(copies, CHIPS)

    turns = lax.axis_size("rep_1")
    pieces = [piece]
    for step in range(1, turns):
        move = [(i, (i - step) % turns) for i in range(turns)]
        pieces.append(lax.ppermute(piece, "rep_1", move))
    w_own = call(
        weight_kernel,
        near(chips + 1, 2 * rows, half, dtype=BF16),
        turn,
        *pieces,
        m_send,
        scalars=1,
    )
    w_own = w_own.reshape(units + 2 * rows, half)
    d_hidden, m_peer = call(
        lambda *refs: hidden_kernel(rows, *refs),
        (far(tokens, units, dtype=BF16), near(rows, half)),
        core_s,
        w_own,
        swap(w_own),
        grad_out,
        scalars=1,
        held=(3,),
        scratch=(
            pltpu.VMEM((tokens, 2 * half), BF16),
            pltpu.SemaphoreType.DMA((2 * half // BLOCK,)),
        ),
    )
    coded, m_peer, d_hidden = lax.optimization_barrier((coded, m_peer, d_hidden))
    halves = (
        pltpu.VMEM((units, half), BF16),
        pltpu.VMEM((units, half), BF16),
        pltpu.SemaphoreType.DMA((2,)),
    )
    high, low, grams = call(
        gram_kernel,
        (
            pltpu.HBM((units, half), BF16),
            pltpu.HBM((units, half), BF16),
            near(rank + units, units),
        ),
        q_t,
        coded,
        kept=(0, 1),
        scratch=halves,
    )
    q_next, update, error = call(
        lambda *refs: last_kernel(n_rep, *refs),
        (far(rank, 2 * half), far(rows, 2 * half), far(rows, 2 * half)),
        core_s,
        row,
        grams,
        q_far,
        swap(coded),
        m_own,
        m_peer,
        high,
        low,
        scalars=2,
        held=(7, 8),
        scratch=halves[:2] * 2 + halves[2:],
    )
    return (update, error[None], q_next.T, d_hidden)


def solution(mesh):
    finer = Mesh(
        mesh.devices.reshape(2, mesh.shape["rep"] // 2, 4, 8, 2), REP_SHARD
    )
    placed = (P(REP_SHARD, None), P(REP_SHARD, None), P(SHARD, None), P(REP, SHARD, None), P())
    return jax.shard_map(
        body,
        mesh=finer,
        in_specs=placed,
        out_specs=(P(SHARD, None), P(REP, SHARD, None), P(), P(REP_SHARD, None)),
        check_vma=False,
    )
```
